256 devices in a mesh: pb: 16 (over z, core), sp: 16 (over y, x).
Axes of the slice: x: 4, y: 4, z: 8, core: 2. Of those that a mesh axis runs over, the one named last changes fastest.
Arguments:
- nodes: bfloat16 [65536, 1024], P(('pb', 'sp')), may hold values from -40 to 40
- project_in: bfloat16 [1024, 3072], replicated, may hold values from -0.3 to 0.3
- project_out: bfloat16 [1024, 1024], replicated, may hold values from -0.1875 to 0.1875
- tile_list: int32 [512, 32], replicated, may hold values from 0 to 511, as said below
- tile_count: int32 [512], replicated, may hold values from 2 to 32, as said below
Outputs:
- mixed: bfloat16 [65536, 1024], P(('pb', 'sp'))
The draws below stay inside these ranges and needn't reach their ends.
Inputs may be any that keep to these rules, and one draw needn't show every extreme that they name: `tile_list`: position 0 of row t is t itself. Over the live positions of the rows of one group (rows g * 32 to (g + 1) * 32 - 1), at most 4 distinct tiles of any other group are listed, and exactly 4 of the next group's tiles (group g + 1, after the last comes the first). A tile may stand more than once in a row. `tile_count`: row 0 has 32.
All inputs are finite; a program needn't handle non-finite values.
Results may differ from the reference program's by a relative error of at most 0.0082.
Values may be sent and summed in bfloat16 or wider, within the bound.
A program may use at most 128 MiB of HBM per device.

```python
import jax
import jax.numpy as jnp
from jax import lax

D = 1024
HEADS = 16
HEAD_DIM = 64
TILE = 128
LISTED = 32
SLOTS = 4
GROUP_TILES = 32
TILES = 512
NODES = 65536


def draw_nodes(key, part):
    keys = jax.random.split(key, 1)
    base = jnp.clip(jax.random.normal(keys[0], (NODES, D), jnp.float32), -6.0, 6.0)
    values_out = base
    return values_out.astype(jnp.bfloat16)


def draw_project_in(key, part):
    fresh = jnp.clip(jax.random.normal(key, (D, HEADS, 3, HEAD_DIM), jnp.float32), -6.0, 6.0) * D ** (-0.5)
    fresh = jnp.clip(fresh, -0.296875, 0.296875)
    return fresh.reshape(D, 3 * D).astype(jnp.bfloat16)


def draw_tile_list(key, part):
    keys = jax.random.split(key, 5)
    groups = TILES // GROUP_TILES
    tile_ids = jnp.arange(TILES, dtype=jnp.int32)
    group_of = tile_ids // GROUP_TILES
    local_of = tile_ids % GROUP_TILES
    pool_base = jax.random.randint(keys[0], (groups, groups), 0, GROUP_TILES, dtype=jnp.int32)
    kinds = jax.random.randint(keys[1], (TILES, LISTED), 0, 4, dtype=jnp.int32)
    offsets = jax.random.randint(keys[2], (TILES, LISTED), -4, 5, dtype=jnp.int32)
    hops = jax.random.randint(keys[3], (TILES, LISTED), 1, groups, dtype=jnp.int32)
    picks = jax.random.randint(keys[4], (TILES, LISTED), 0, SLOTS, dtype=jnp.int32)
    nearby = group_of[:, None] * GROUP_TILES + (local_of[:, None] + offsets) % GROUP_TILES
    owners = (group_of[:, None] + hops) % groups
    faraway = owners * GROUP_TILES + (pool_base[group_of[:, None], owners] + picks) % GROUP_TILES
    entries = jnp.where(kinds == 3, faraway, nearby)
    next_owner = (group_of + 1) % groups
    forced = next_owner * GROUP_TILES + (pool_base[group_of, next_owner] + local_of % SLOTS) % GROUP_TILES
    columns = jnp.arange(LISTED, dtype=jnp.int32)[None, :]
    entries = jnp.where(columns == 0, tile_ids[:, None], jnp.where(columns == 1, forced[:, None], entries))
    return entries.astype(jnp.int32)


def draw_tile_count(key, part):
    keys = jax.random.split(key, 2)
    groups = TILES // GROUP_TILES
    tile_ids = jnp.arange(TILES, dtype=jnp.int32)
    row_draw = jax.random.randint(keys[0], (TILES,), 0, 31, dtype=jnp.int32)
    group_draw = jax.random.randint(keys[1], (groups,), 15, 31, dtype=jnp.int32)
    counts = 2 + row_draw * group_draw[tile_ids // GROUP_TILES] * (LISTED - 2) // 900
    counts = jnp.where(tile_ids == 0, LISTED, counts)
    return counts.astype(jnp.int32)


def normal_values(stream_key, dims, scale, reach, held_as=jnp.bfloat16):
    drawn = scale * jax.random.normal(stream_key, dims, jnp.float32)
    return jnp.clip(drawn, min=-reach, max=reach).astype(held_as)


def setup_inputs(seed: int = 0) -> dict:
    streams_of = jax.random.split(jax.random.key(seed), 6)
    return {
        "nodes": draw_nodes(jax.random.fold_in(streams_of[5], 71), 0),
        "project_in": draw_project_in(jax.random.fold_in(streams_of[5], 71), 0),
        "project_out": normal_values(streams_of[2], (D, D), D ** -0.5, 0.1875),
        "tile_list": draw_tile_list(jax.random.fold_in(streams_of[5], 71), 0),
        "tile_count": draw_tile_count(jax.random.fold_in(streams_of[5], 71), 0),
    }


NEGATIVE = -1.0e30


def live_mask(tile_list, tile_count):
    listed = tile_list.shape[1]
    places = jnp.arange(listed, dtype=jnp.int32)
    inside = places[None, :] < tile_count[:, None]
    earlier = (places[:, None] > places[None, :])[None, :, :]
    repeats = (tile_list[:, :, None] == tile_list[:, None, :]) & earlier
    return inside & jnp.logical_not(jnp.any(repeats, axis=2))


def reference(nodes, project_in, project_out, tile_list, tile_count):
    all_tiles = tile_list.shape[0]
    node_tiles = nodes.reshape(all_tiles, TILE, D)

    def project_tile(block_nodes):
        return jnp.dot(block_nodes, project_in, preferred_element_type=jnp.float32).astype(jnp.bfloat16)

    projected = lax.map(project_tile, node_tiles).reshape(all_tiles, TILE, HEADS, 3, HEAD_DIM)
    queries = projected[:, :, :, 0]
    keys_all = projected[:, :, :, 1]
    values_all = projected[:, :, :, 2]
    usable = live_mask(tile_list, tile_count)
    score_scale = HEAD_DIM ** -0.5

    def attend_tile(packed):
        query_tile, chosen, allowed = packed
        fetched_keys = keys_all[chosen].astype(jnp.float32)
        fetched_values = values_all[chosen].astype(jnp.float32)
        scores = jnp.einsum("bhe,jkhe->hbjk", query_tile.astype(jnp.float32), fetched_keys) * score_scale
        allowed_mask = allowed[None, None, :, None]
        scores = jnp.where(allowed_mask, scores, NEGATIVE)
        highest = jnp.max(scores, axis=(2, 3), keepdims=True)
        weights = jnp.where(allowed_mask, jnp.exp(scores - highest), 0.0)
        running_total = jnp.sum(weights, axis=(2, 3))
        rounded = lax.optimization_barrier(weights.astype(jnp.bfloat16)).astype(jnp.float32)
        summed = jnp.einsum("hbjk,jkhe->bhe", rounded, fetched_values)
        return (summed / jnp.transpose(running_total)[:, :, None]).astype(jnp.bfloat16)

    attended = lax.map(attend_tile, (queries, tile_list, usable)).reshape(all_tiles, TILE, D)

    def finish_tile(packed):
        node_block, attended_block = packed
        added = node_block.astype(jnp.float32) + jnp.dot(attended_block, project_out, preferred_element_type=jnp.float32)
        return added.astype(jnp.bfloat16)

    mixed_out = lax.map(finish_tile, (node_tiles, attended)).reshape(NODES, D)
    return mixed_out
```

```python
import functools

import jax
import jax.numpy as jnp
from jax import lax
from jax.experimental import pallas as pl
from jax.experimental.pallas import tpu as pltpu
from jax.sharding import PartitionSpec as P

D = 1024
HEADS = 16
HEAD_DIM = 64
TILE = 128
LISTED = 32
SLOTS = 4
GROUP = 32
N = 16
CHUNK = 4
LOW = -1e30
MESH = pl.DeviceIdType.MESH


def tables(tile_list, tile_count):
    g = lax.axis_index("pb")
    places = jnp.arange(LISTED, dtype=jnp.int32)
    marked = jnp.where(places[None, :] < tile_count[:, None], tile_list, -1)
    local = marked - g * GROUP
    mine = jnp.arange(GROUP, dtype=jnp.int32)
    used = jnp.any(local.reshape(N, GROUP * LISTED, 1) == mine, axis=1)
    rank = jnp.sum(used[:, None, :] & (mine[None, :] < mine[:, None])[None], axis=2)
    slot = jnp.arange(SLOTS, dtype=jnp.int32)
    hit = used[:, None, :] & (rank[:, None, :] == slot[None, :, None])
    send = jnp.sum(jnp.where(hit, mine, 0), axis=2).reshape(N * SLOTS)
    own = lax.dynamic_slice_in_dim(marked, g * GROUP, GROUP, 0)
    tiles = jnp.arange(N * GROUP, dtype=jnp.int32)
    wanted = jnp.any(own.reshape(-1, 1) == tiles, axis=0).reshape(N, GROUP)
    wrank = jnp.sum(wanted[:, None, :] & (mine[None, :] < mine[:, None])[None], axis=2)
    whit = wanted[:, None, :] & (wrank[:, None, :] == slot[None, :, None])
    ids = jnp.sum(jnp.where(whit, mine + 1, 0), axis=2)
    base = jnp.arange(N, dtype=jnp.int32)[:, None] * GROUP
    usable = (ids > 0) & (jnp.arange(N)[:, None] != g)
    remote_ids = jnp.where(usable, ids - 1 + base, -2).reshape(N * SLOTS)
    slot_tile = jnp.concatenate([mine + g * GROUP, remote_ids])
    count_slots = slot_tile.shape[0]
    present = jnp.any(own[:, None, :] == slot_tile[None, :, None], axis=2)
    every = jnp.arange(count_slots, dtype=jnp.int32)
    prank = jnp.sum(present[:, None, :] & (every[None, :] < every[:, None])[None], axis=2)
    phit = present[:, None, :] & (prank[:, None, :] == places[None, :, None])
    slots = jnp.sum(jnp.where(phit, every, 0), axis=2)
    counts = jnp.sum(present, axis=1)
    return send.astype(jnp.int32), slots.astype(jnp.int32), counts.astype(jnp.int32)


def exchange_kernel(
    send_ref, nodes_ref, w_hbm, q_out, kv_out, far_out,
    w_buf, kv_send, q_send, far_send, w_sem, kv_ss, kv_rs, q_ss, q_rs, z_ss, z_rs, l_sem,
):
    me = lax.axis_index("sp")
    grp = lax.axis_index("pb")

    def w_copy(p):
        cols = pl.ds(pl.multiple_of(p * 384, 128), 384)
        return pltpu.make_async_copy(w_hbm.at[:, cols], w_buf.at[p], w_sem.at[p])

    def pair(i):
        return lax.rem(me // 2 + i, 8)

    for i in range(8):
        w_copy(pair(i)).start()

    barrier = pltpu.get_barrier_semaphore()

    def greet(d, _):
        pl.semaphore_signal(barrier, inc=1, device_id={"sp": lax.rem(me + d, N)}, device_id_type=MESH)
        pl.semaphore_signal(barrier, inc=1, device_id={"pb": lax.rem(grp + d, N)}, device_id_type=MESH)
        return 0

    lax.fori_loop(1, N, greet, 0)
    pl.semaphore_wait(barrier, 2 * (N - 1))

    def kv_copy(src, dst, idx):
        return pltpu.make_async_remote_copy(
            src_ref=kv_send.at[dst], dst_ref=kv_out.at[idx], send_sem=kv_ss.at[dst],
            recv_sem=kv_rs.at[idx], device_id={"sp": dst}, device_id_type=MESH)

    def q_copy(dst, idx):
        return pltpu.make_async_remote_copy(
            src_ref=q_send.at[dst], dst_ref=q_out.at[idx], send_sem=q_ss.at[dst],
            recv_sem=q_rs.at[idx], device_id={"sp": dst}, device_id_type=MESH)

    def project(i, _):
        p = pair(i)
        w_copy(p).wait()
        y = jnp.dot(nodes_ref[...], w_buf[p], preferred_element_type=jnp.float32)
        for k in range(2):
            h = 2 * p + k
            o = k * 192
            q = (y[:, o:o + 64] * HEAD_DIM ** -0.5).astype(jnp.bfloat16)
            kv_send[h] = y[:, o + 64:o + 192].astype(jnp.bfloat16)
            q_send[h] = jnp.concatenate([q[:TILE], q[TILE:]], axis=1)

            @pl.when(h != me)
            def _():
                kv_copy(me, h, me).start()
        return 0

    lax.fori_loop(0, 8, project, 0)
    kv_out[me] = kv_send[me]
    q_out[me] = q_send[me]

    def send_q(d, _):
        q_copy(lax.rem(me + d, N), me).start()
        return 0

    lax.fori_loop(1, N, send_q, 0)

    def wait_kv(d, _):
        s = lax.rem(me + N - d, N)
        kv_copy(me, s, s).wait_recv()
        return 0

    lax.fori_loop(1, N, wait_kv, 0)

    def far_copy(dst, idx):
        return pltpu.make_async_remote_copy(
            src_ref=far_send.at[dst], dst_ref=far_out.at[idx], send_sem=z_ss.at[dst],
            recv_sem=z_rs.at[idx], device_id={"pb": dst}, device_id_type=MESH)

    def select(d, _):
        half = lax.div(d + 1, 2)
        off = 8 + half * (2 * lax.rem(d, 2) - 1)
        dst = lax.rem(grp + off, N)
        for k in range(SLOTS):
            t = send_ref[dst * SLOTS + k]
            far_send[dst, k * TILE:(k + 1) * TILE] = kv_out[lax.div(t, 2), pl.ds(lax.rem(t, 2) * TILE, TILE)]
        far_copy(dst, grp).start()
        return 0

    lax.fori_loop(0, N - 1, select, 0)
    far_out[grp] = kv_out[0:2].reshape(4 * TILE, TILE)

    def drain(d, _):
        s = lax.rem(me + N - d, N)
        q_copy(s, s).wait_recv()
        q_copy(s, s).wait_send()
        kv_copy(me, s, s).wait_send()
        return 0

    lax.fori_loop(1, N, drain, 0)

    def drain_far(d, _):
        s = lax.rem(grp + N - d, N)
        far_copy(s, s).wait_recv()
        far_copy(s, s).wait_send()
        return 0

    lax.fori_loop(1, N, drain_far, 0)


def exchange(send, nodes, project_in):
    b16 = jnp.bfloat16
    vm = pl.BlockSpec(memory_space=pltpu.VMEM)
    dma = pltpu.SemaphoreType.DMA
    return pl.pallas_call(
        exchange_kernel,
        out_shape=(
            jax.ShapeDtypeStruct((N, TILE, TILE), b16),
            jax.ShapeDtypeStruct((N, 2 * TILE, TILE), b16),
            jax.ShapeDtypeStruct((N, SLOTS * TILE, TILE), b16),
        ),
        in_specs=[pl.BlockSpec(memory_space=pltpu.SMEM), vm, pl.BlockSpec(memory_space=pl.ANY)],
        out_specs=(vm, vm, vm),
        scratch_shapes=[
            pltpu.VMEM((8, D, 384), b16),
            pltpu.VMEM((N, 2 * TILE, TILE), b16),
            pltpu.VMEM((N, TILE, TILE), b16),
            pltpu.VMEM((N, SLOTS * TILE, TILE), b16),
            dma((8,)), dma((N,)), dma((N,)), dma((N,)), dma((N,)), dma((N,)), dma((N,)), dma,
        ],
        compiler_params=pltpu.CompilerParams(
            collective_id=0, has_side_effects=True, vmem_limit_bytes=40 << 20),
        name="exchange",
    )(send, nodes, project_in)


def attend_kernel(
    slots_ref, counts_ref, q_ref, kv_ref, far_ref, out_ref,
    kv, qz, acc, total, top, s_buf, p_buf, m_cur, m_max, a_cur, a_old,
):
    kv[0:GROUP] = kv_ref[...].reshape(GROUP, TILE, TILE)
    kv[GROUP:] = far_ref[...].reshape(N * SLOTS, TILE, TILE)
    lane = lax.broadcasted_iota(jnp.int32, (TILE, TILE), 1)
    zero64 = jnp.zeros((TILE, HEAD_DIM), jnp.bfloat16)

    def setup(s, _):
        both = q_ref[s]
        qz[2 * s] = jnp.concatenate([both[:, :HEAD_DIM], zero64], axis=1)
        qz[2 * s + 1] = jnp.concatenate([both[:, HEAD_DIM:], zero64], axis=1)
        return 0

    lax.fori_loop(0, N, setup, 0)

    def clear(r, _):
        acc[r] = jnp.zeros((TILE, TILE), jnp.float32)
        total[r] = jnp.zeros((TILE, TILE), jnp.float32)
        top[r] = jnp.full((TILE, TILE), LOW, jnp.float32)
        return 0

    lax.fori_loop(0, GROUP + 1, clear, 0)
    s_buf[...] = jnp.zeros_like(s_buf)
    p_buf[...] = jnp.zeros_like(p_buf)
    m_cur[...] = jnp.zeros_like(m_cur)
    m_max[...] = jnp.zeros_like(m_max)
    a_cur[...] = jnp.zeros_like(a_cur)
    a_old[...] = jnp.zeros_like(a_old)

    def chunks_of(r):
        return jnp.maximum(lax.div(counts_ref[r] + CHUNK - 1, CHUNK), 1)

    items = lax.fori_loop(0, GROUP, lambda r, n: n + chunks_of(r), 0)

    def fetch(r, c):
        row = jnp.minimum(r, GROUP - 1)
        return jnp.concatenate([kv[slots_ref[row, c * CHUNK + t]] for t in range(CHUNK)], axis=0)

    def advance(i, state):
        r0, c0, r1, c1, r2, c2, r3, c3 = state
        added = jnp.dot(p_buf[...], fetch(r3, c3), preferred_element_type=jnp.float32)
        acc[r3] = acc[r3] * a_old[...] + added
        slot = lax.rem(i, 2)
        m = m_cur[...]
        fade = a_cur[...]
        part = None
        for t in range(CHUNK):
            cols = slice(t * TILE, (t + 1) * TILE)
            w = jnp.exp(s_buf[slot, :, cols] - m)
            p_buf[:, cols] = w.astype(jnp.bfloat16)
            part = w if part is None else part + w
        total[r2] = total[r2] * fade + part
        a_old[...] = fade
        before = top[r1]
        now = jnp.maximum(before, jnp.max(m_max[...], axis=1, keepdims=True))
        top[r1] = now
        m_cur[...] = now
        a_cur[...] = jnp.exp(before - now)
        row = jnp.minimum(r0, GROUP - 1)
        s = lax.dot_general(
            qz[row], fetch(r0, c0), (((1,), (1,)), ((), ())), preferred_element_type=jnp.float32)
        live = counts_ref[row]
        big = None
        for t in range(CHUNK):
            cols = slice(t * TILE, (t + 1) * TILE)
            bias = jnp.where(c0 * CHUNK + t < live, 0.0, LOW)
            st = s[:, cols] + bias
            s_buf[slot, :, cols] = st
            big = st if big is None else jnp.maximum(big, st)
        m_max[...] = big
        more = (c0 + 1 < chunks_of(row)) & (r0 < GROUP)
        rn = jnp.where(more, r0, jnp.minimum(r0 + 1, GROUP))
        cn = jnp.where(more, c0 + 1, 0)
        return rn, cn, r0, c0, r1, c1, r2, c2

    start = (0, 0, GROUP, 0, GROUP, 0, GROUP, 0)
    lax.fori_loop(0, items + 3, advance, tuple(jnp.int32(v) for v in start))

    def finish(s, _):
        even = acc[2 * s] / jnp.sum(total[2 * s], axis=1, keepdims=True)
        odd = acc[2 * s + 1] / jnp.sum(total[2 * s + 1], axis=1, keepdims=True)
        even = pltpu.roll(even, HEAD_DIM, 1)
        out_ref[s] = jnp.where(lane < HEAD_DIM, even, odd).astype(jnp.bfloat16)
        return 0

    lax.fori_loop(0, N, finish, 0)


def attend(slots, counts, q, kv, far):
    b16, f32 = jnp.bfloat16, jnp.float32
    vm = pl.BlockSpec(memory_space=pltpu.VMEM)
    sm = pl.BlockSpec(memory_space=pltpu.SMEM)
    square = pltpu.VMEM((TILE, TILE), f32)
    return pl.pallas_call(
        attend_kernel,
        out_shape=jax.ShapeDtypeStruct((N, TILE, TILE), b16),
        in_specs=[sm, sm, vm, vm, vm],
        out_specs=vm,
        scratch_shapes=[
            pltpu.VMEM((GROUP + N * SLOTS, TILE, TILE), b16),
            pltpu.VMEM((GROUP, TILE, TILE), b16),
            pltpu.VMEM((GROUP + 1, TILE, TILE), f32),
            pltpu.VMEM((GROUP + 1, TILE, TILE), f32),
            pltpu.VMEM((GROUP + 1, TILE, TILE), f32),
            pltpu.VMEM((2, TILE, CHUNK * TILE), f32),
            pltpu.VMEM((TILE, CHUNK * TILE), b16),
            square, square, square, square,
        ],
        compiler_params=pltpu.CompilerParams(vmem_limit_bytes=40 << 20),
        name="attend",
    )(slots, counts, q, kv, far)


def finish_kernel(att_ref, nodes_ref, w_ref, out_ref, got, joined, ss, rs):
    me = lax.axis_index("sp")
    barrier = pltpu.get_barrier_semaphore()

    def greet(d, _):
        pl.semaphore_signal(barrier, inc=1, device_id={"sp": lax.rem(me + d, N)}, device_id_type=MESH)
        return 0

    lax.fori_loop(1, N, greet, 0)
    pl.semaphore_wait(barrier, N - 1)

    def copy(dst, idx):
        return pltpu.make_async_remote_copy(
            src_ref=att_ref.at[dst], dst_ref=got.at[idx], send_sem=ss.at[dst],
            recv_sem=rs.at[idx], device_id={"sp": dst}, device_id_type=MESH)

    def send(d, _):
        copy(lax.rem(me + d, N), me).start()
        return 0

    lax.fori_loop(1, N, send, 0)
    got[me] = att_ref[me]

    def drain(d, _):
        s = lax.rem(me + N - d, N)
        copy(s, s).wait_recv()
        copy(s, s).wait_send()
        return 0

    lax.fori_loop(1, N, drain, 0)
    for p in range(HEADS // 2):
        a, b = got[2 * p], got[2 * p + 1]
        cols = slice(p * TILE, (p + 1) * TILE)
        joined[:TILE, cols] = jnp.concatenate([a[:, :HEAD_DIM], b[:, :HEAD_DIM]], axis=1)
        joined[TILE:, cols] = jnp.concatenate([a[:, HEAD_DIM:], b[:, HEAD_DIM:]], axis=1)
    for c in range(4):
        cols = slice(c * 256, (c + 1) * 256)
        y = jnp.dot(joined[...], w_ref[:, cols], preferred_element_type=jnp.float32)
        out_ref[:, cols] = (nodes_ref[:, cols].astype(jnp.float32) + y).astype(jnp.bfloat16)


def finish(att, nodes, project_out):
    b16 = jnp.bfloat16
    vm = pl.BlockSpec(memory_space=pltpu.VMEM)
    dma = pltpu.SemaphoreType.DMA
    return pl.pallas_call(
        finish_kernel,
        out_shape=jax.ShapeDtypeStruct((2 * TILE, D), b16),
        in_specs=[vm, vm, vm],
        out_specs=vm,
        scratch_shapes=[
            pltpu.VMEM((N, TILE, TILE), b16),
            pltpu.VMEM((2 * TILE, D), b16),
            dma((N,)), dma((N,)),
        ],
        compiler_params=pltpu.CompilerParams(
            collective_id=1, has_side_effects=True, vmem_limit_bytes=40 << 20),
        name="finish",
    )(att, nodes, project_out)


def shards(nodes, project_in, project_out, tile_list, tile_count):
    send, slots, counts = tables(tile_list, tile_count)
    q, kv, far = exchange(send, nodes, project_in)
    att = attend(slots, counts, q, kv, far)
    return finish(att, nodes, project_out)


def solution(mesh):
    in_specs = (P(("pb", "sp"), None), P(), P(), P(), P())
    out_specs = P(("pb", "sp"), None)
    return jax.shard_map(shards, mesh=mesh, in_specs=in_specs, out_specs=out_specs, check_vma=False)
```

```python
import functools

import jax
import jax.numpy as jnp
from jax import lax
from jax.experimental import pallas as pl
from jax.experimental.pallas import tpu as pltpu
from jax.sharding import PartitionSpec as P

D = 1024
HEADS = 16
HEAD_DIM = 64
TILE = 128
LISTED = 32
SLOTS = 4
GROUP = 32
N = 16
CHUNK = 4
EARLY = 12
LOW = -1e30
MESH = pl.DeviceIdType.MESH


def build_tables(list_ref, count_ref, marked_ref, tab_ref, grp):
    f32, b16, i32 = jnp.float32, jnp.bfloat16, jnp.int32
    base = grp * GROUP
    places = lax.broadcasted_iota(i32, (LISTED, N * GROUP), 0)
    across = jnp.where(places < count_ref[...], list_ref[...], -1)
    for b in range(0, N * GROUP, TILE):
        marked_ref[b:b + TILE, :] = across[:, b:b + TILE].T
    lane = lax.broadcasted_iota(i32, (N, TILE), 1)

    def uses(i, used):
        hit = jnp.where(marked_ref[...] == base + i, 1.0, 0.0)
        hit = jnp.max(hit.reshape(N, GROUP, LISTED), axis=1)
        return jnp.where(lane == i, jnp.max(hit, axis=1, keepdims=True), used)

    used = lax.fori_loop(0, GROUP, uses, jnp.zeros((N, TILE), f32), unroll=4)
    low = lax.broadcasted_iota(i32, (TILE, TILE), 0) < lax.broadcasted_iota(i32, (TILE, TILE), 1)
    rank = jnp.dot(used.astype(b16), jnp.where(low, 1.0, 0.0).astype(b16), preferred_element_type=f32)
    send = jnp.zeros((N, TILE), f32)
    for k in range(SLOTS):
        pick = jnp.where((rank == k) & (used > 0), lane.astype(f32), 0.0)
        send = jnp.where(lane == k, jnp.sum(pick, axis=1, keepdims=True), send)
    tab_ref[GROUP:] = send.astype(i32)
    tiles = N * GROUP
    own = marked_ref[pl.ds(pl.multiple_of(base, GROUP), GROUP), :]
    tile = lax.broadcasted_iota(i32, (GROUP, tiles), 1)
    present = jnp.zeros((GROUP, tiles), f32)
    for j in range(LISTED):
        present = jnp.where(own[:, j:j + 1] == tile, 1.0, present)
    up = lax.broadcasted_iota(i32, (tiles, tiles), 0)
    across = lax.broadcasted_iota(i32, (tiles, tiles), 1)
    before = up < across
    same = before & (lax.div(up, GROUP) == lax.div(across, GROUP))
    before = jnp.where(before, 1.0, 0.0).astype(b16)
    same = jnp.where(same, 1.0, 0.0).astype(b16)
    wanted = jnp.broadcast_to(jnp.max(present, axis=0, keepdims=True), (N, tiles))
    rank = jnp.dot(wanted.astype(b16), same, preferred_element_type=f32)[0:1]
    owner = lax.div(tile, GROUP)
    here = owner == grp
    slot = jnp.where(here, (tile - base).astype(f32), (GROUP + SLOTS * owner).astype(f32) + rank)
    near = jnp.where(here, present, 0.0)
    away = jnp.where(here, 0.0, present)
    both = jnp.concatenate([near, away], axis=0).astype(b16)
    order = jnp.dot(both, before, preferred_element_type=f32)
    near_count = jnp.sum(near, axis=1, keepdims=True)
    count = jnp.sum(present, axis=1, keepdims=True)
    order = jnp.where(here, order[:GROUP], order[GROUP:] + near_count)
    order = jnp.where(present > 0, order, -1.0)
    wide = lax.broadcasted_iota(i32, (GROUP, TILE), 1)

    def place(k, out):
        v = jnp.sum(jnp.where(order == k.astype(f32), slot, 0.0), axis=1, keepdims=True)
        return jnp.where(wide == k, v, out)

    out = lax.fori_loop(0, LISTED, place, jnp.zeros((GROUP, TILE), f32), unroll=4)
    out = jnp.where(wide == LISTED, near_count, out)
    out = jnp.where(wide == LISTED + 1, count, out)
    tab_ref[:GROUP] = out.astype(i32)


def scratch_state():
    f32 = jnp.float32
    square = pltpu.VMEM((TILE, TILE), f32)
    return [
        pltpu.VMEM((2, TILE, CHUNK * TILE), f32),
        pltpu.VMEM((TILE, CHUNK * TILE), jnp.bfloat16),
        square, square, square, square,
    ]


def clear_stages(s_buf, p_buf, m_cur, m_max, a_cur, a_old):
    for ref in (s_buf, p_buf, m_cur, m_max, a_cur, a_old):
        ref[...] = jnp.zeros_like(ref)


def run_stages(slot, items, fetch, live, qz, state, buffers):
    acc, total, top = state
    s_buf, p_buf, m_cur, m_max, a_cur, a_old = buffers
    (r0, c0), (r1, _), (r2, _), (r3, c3) = items
    added = jnp.dot(p_buf[...], fetch(r3, c3), preferred_element_type=jnp.float32)
    acc[r3] = acc[r3] * a_old[...] + added
    m = m_cur[...]
    fade = a_cur[...]
    part = None
    for t in range(CHUNK):
        cols = slice(t * TILE, (t + 1) * TILE)
        w = jnp.exp(s_buf[slot, :, cols] - m)
        p_buf[:, cols] = w.astype(jnp.bfloat16)
        part = w if part is None else part + w
    total[r2] = total[r2] * fade + part
    a_old[...] = fade
    before = top[r1]
    now = jnp.maximum(before, jnp.max(m_max[...], axis=1, keepdims=True))
    top[r1] = now
    m_cur[...] = now
    a_cur[...] = jnp.exp(before - now)
    row = jnp.minimum(r0, GROUP - 1)
    s = lax.dot_general(
        qz[row], fetch(r0, c0), (((1,), (1,)), ((), ())), preferred_element_type=jnp.float32)
    big = None
    for t in range(CHUNK):
        cols = slice(t * TILE, (t + 1) * TILE)
        st = s[:, cols] + jnp.where(c0 + t < live(row), 0.0, LOW)
        s_buf[slot, :, cols] = st
        big = st if big is None else jnp.maximum(big, st)
    m_max[...] = big


def exchange_kernel(
    list_hbm, count_hbm, nodes_hbm, w_hbm, qz, kv_out, far_out, tab_out, acc, total, top,
    w_buf, kv_send, q_send, q_got, far_send, list_ref, count_ref, nodes_ref, marked, tab, in_sem, w_sem, kv_ss, kv_rs, q_ss, q_rs, z_ss, z_rs, t_sem,
    *buffers,
):
    me = lax.axis_index("sp")
    grp = lax.axis_index("pb")

    def w_copy(p):
        cols = pl.ds(pl.multiple_of(p * 384, 128), 384)
        return pltpu.make_async_copy(w_hbm.at[:, cols], w_buf.at[p], w_sem.at[p])

    def pair(i):
        return lax.rem(me // 2 + i, 8)

    arrivals = [
        pltpu.make_async_copy(a, b, in_sem.at[i])
        for i, (a, b) in enumerate(((nodes_hbm, nodes_ref), (list_hbm, list_ref), (count_hbm, count_ref)))
    ]
    for copy in arrivals:
        copy.start()
    for i in range(8):
        w_copy(pair(i)).start()

    barrier = pltpu.get_barrier_semaphore()

    def greet(d, _):
        pl.semaphore_signal(barrier, inc=1, device_id={"sp": lax.rem(me + d, N)}, device_id_type=MESH)
        pl.semaphore_signal(barrier, inc=1, device_id={"pb": lax.rem(grp + d, N)}, device_id_type=MESH)
        return 0

    lax.fori_loop(1, N, greet, 0)
    pl.semaphore_wait(barrier, 2 * (N - 1))

    def kv_copy(src, dst, idx):
        return pltpu.make_async_remote_copy(
            src_ref=kv_send.at[dst], dst_ref=kv_out.at[pl.ds(2 * idx, 2)], send_sem=kv_ss.at[dst],
            recv_sem=kv_rs.at[idx], device_id={"sp": dst}, device_id_type=MESH)

    def q_copy(dst, idx):
        return pltpu.make_async_remote_copy(
            src_ref=q_send.at[dst], dst_ref=q_got.at[idx], send_sem=q_ss.at[dst],
            recv_sem=q_rs.at[idx], device_id={"sp": dst}, device_id_type=MESH)

    def project(i, _):
        p = pair(i)
        w_copy(p).wait()
        y = jnp.dot(nodes_ref[...], w_buf[p], preferred_element_type=jnp.float32)
        for k in range(2):
            h = 2 * p + k
            o = k * 192
            q = (y[:, o:o + 64] * HEAD_DIM ** -0.5).astype(jnp.bfloat16)
            kv_send[h] = y[:, o + 64:o + 192].astype(jnp.bfloat16).reshape(2, TILE, TILE)
            q_send[h] = jnp.concatenate([q[:TILE], q[TILE:]], axis=1)

            @pl.when(h != me)
            def _():
                kv_copy(me, h, me).start()
        return 0

    for copy in arrivals:
        copy.wait()
    lax.fori_loop(0, 8, project, 0)
    kv_out[pl.ds(2 * me, 2)] = kv_send[me]
    q_got[me] = q_send[me]

    def send_q(d, _):
        q_copy(lax.rem(me + d, N), me).start()
        return 0

    lax.fori_loop(1, N, send_q, 0)

    build_tables(list_ref, count_ref, marked, tab_out, grp)
    to_scalar = pltpu.make_async_copy(tab_out, tab, t_sem)
    to_scalar.start()

    def clear(r, _):
        acc[r] = jnp.zeros((TILE, TILE), jnp.float32)
        total[r] = jnp.zeros((TILE, TILE), jnp.float32)
        top[r] = jnp.full((TILE, TILE), LOW, jnp.float32)
        return 0

    lax.fori_loop(0, GROUP + 1, clear, 0)
    clear_stages(*buffers)
    to_scalar.wait()

    def wait_kv(d, _):
        s = lax.rem(me + N - d, N)
        kv_copy(me, s, s).wait_recv()
        return 0

    lax.fori_loop(1, N, wait_kv, 0)

    def far_copy(dst, idx):
        return pltpu.make_async_remote_copy(
            src_ref=far_send.at[dst], dst_ref=far_out.at[pl.ds(SLOTS * idx, SLOTS)], send_sem=z_ss.at[dst],
            recv_sem=z_rs.at[idx], device_id={"pb": dst}, device_id_type=MESH)

    def select(d, _):
        half = lax.div(d + 1, 2)
        off = 8 + half * (2 * lax.rem(d, 2) - 1)
        dst = lax.rem(grp + off, N)
        for k in range(SLOTS):
            far_send[dst, k] = kv_out[jnp.clip(tab[GROUP + dst, k], 0, GROUP - 1)]
        far_copy(dst, grp).start()
        return 0

    lax.fori_loop(0, N - 1, select, 0)
    far_out[pl.ds(SLOTS * grp, SLOTS)] = kv_out[0:SLOTS]

    def drain(d, _):
        s = lax.rem(me + N - d, N)
        q_copy(s, s).wait_recv()
        q_copy(s, s).wait_send()
        kv_copy(me, s, s).wait_send()
        return 0

    lax.fori_loop(1, N, drain, 0)
    zero64 = jnp.zeros((TILE, HEAD_DIM), jnp.bfloat16)

    def setup(s, _):
        both = q_got[s]
        qz[2 * s] = jnp.concatenate([both[:, :HEAD_DIM], zero64], axis=1)
        qz[2 * s + 1] = jnp.concatenate([both[:, HEAD_DIM:], zero64], axis=1)
        return 0

    lax.fori_loop(0, N, setup, 0)

    def fetch(r, c):
        row = jnp.minimum(r, GROUP - 1)
        return jnp.concatenate(
            [kv_out[jnp.clip(tab[row, c + t], 0, GROUP - 1)] for t in range(CHUNK)], axis=0)

    per_row = EARLY // CHUNK
    steps = GROUP * per_row

    def item(i):
        valid = (i >= 0) & (i < steps)
        i = jnp.clip(i, 0, steps - 1)
        row = lax.div(i, per_row)
        return jnp.where(valid, row, GROUP), (i - row * per_row) * CHUNK

    def advance(i, _):
        run_stages(
            lax.rem(i, 2), [item(i - k) for k in range(4)], fetch,
            lambda row: tab[row, LISTED], qz, (acc, total, top), buffers)
        return 0

    lax.fori_loop(0, steps + 3, advance, 0)

    def drain_far(d, _):
        s = lax.rem(grp + N - d, N)
        far_copy(s, s).wait_recv()
        far_copy(s, s).wait_send()
        return 0

    lax.fori_loop(1, N, drain_far, 0)


def exchange(listed, count, nodes, project_in):
    b16, f32, i32 = jnp.bfloat16, jnp.float32, jnp.int32
    vm = pl.BlockSpec(memory_space=pltpu.VMEM)
    dma = pltpu.SemaphoreType.DMA
    state = jax.ShapeDtypeStruct((GROUP + 1, TILE, TILE), f32)
    return pl.pallas_call(
        exchange_kernel,
        out_shape=(
            jax.ShapeDtypeStruct((GROUP, TILE, TILE), b16),
            jax.ShapeDtypeStruct((GROUP, TILE, TILE), b16),
            jax.ShapeDtypeStruct((N * SLOTS, TILE, TILE), b16),
            jax.ShapeDtypeStruct((GROUP + N, TILE), i32),
            state, state, state,
        ),
        in_specs=[pl.BlockSpec(memory_space=pltpu.HBM)] * 4,
        out_specs=(vm,) * 7,
        scratch_shapes=[
            pltpu.VMEM((8, D, 384), b16),
            pltpu.VMEM((N, 2, TILE, TILE), b16),
            pltpu.VMEM((N, TILE, TILE), b16),
            pltpu.VMEM((N, TILE, TILE), b16),
            pltpu.VMEM((N, SLOTS, TILE, TILE), b16),
            pltpu.VMEM((LISTED, N * GROUP), i32),
            pltpu.VMEM((1, N * GROUP), i32),
            pltpu.VMEM((2 * TILE, D), b16),
            pltpu.VMEM((N * GROUP, LISTED), i32),
            pltpu.SMEM((GROUP + N, TILE), i32),
            dma((3,)), dma((8,)), dma((N,)), dma((N,)), dma((N,)), dma((N,)), dma((N,)), dma((N,)), dma,
            *scratch_state(),
        ],
        compiler_params=pltpu.CompilerParams(
            collective_id=0, has_side_effects=True, vmem_limit_bytes=30 << 20),
        name="exchange",
    )(listed, count, nodes, project_in)


def attend_kernel(
    tab, qz, kv_ref, far_ref, acc_in, total_in, top_in, out_ref, acc, total, top, kv, rows, *buffers,
):
    kv[0:GROUP] = kv_ref[...]
    kv[GROUP:] = far_ref[...]
    lane = lax.broadcasted_iota(jnp.int32, (TILE, TILE), 1)
    clear_stages(*buffers)

    def first(r):
        return jnp.minimum(tab[r, LISTED], EARLY)

    def gather(r, carry):
        n, items = carry
        left = tab[r, LISTED + 1] - first(r)
        rows[n] = r
        return n + jnp.where(left > 0, 1, 0), items + lax.div(left + CHUNK - 1, CHUNK)

    used, items = lax.fori_loop(0, GROUP, gather, (jnp.int32(0), jnp.int32(0)))
    rows[used] = GROUP

    def fetch(r, c):
        row = jnp.minimum(r, GROUP - 1)
        return jnp.concatenate(
            [kv[tab[row, jnp.minimum(c + t, LISTED - 1)]] for t in range(CHUNK)], axis=0)

    def advance(i, state):
        n, r0, c0, r1, c1, r2, c2, r3, c3 = state
        run_stages(
            lax.rem(i, 2), ((r0, c0), (r1, c1), (r2, c2), (r3, c3)), fetch,
            lambda row: tab[row, LISTED + 1], qz, (acc, total, top), buffers)
        row = jnp.minimum(r0, GROUP - 1)
        more = (c0 + CHUNK < tab[row, LISTED + 1]) & (r0 < GROUP)
        n = jnp.where(more, n, jnp.minimum(n + 1, used))
        rn = jnp.where(more, r0, rows[n])
        cn = jnp.where(more, c0 + CHUNK, first(jnp.minimum(rn, GROUP - 1)))
        return n, rn, cn, r0, c0, r1, c1, r2, c2

    r = rows[0]
    zero, dummy = jnp.int32(0), jnp.int32(GROUP)
    start = (zero, r, first(jnp.minimum(r, GROUP - 1)), dummy, zero, dummy, zero, dummy, zero)
    lax.fori_loop(0, items + 3, advance, start)

    def finish(s, _):
        even = acc[2 * s] / jnp.sum(total[2 * s], axis=1, keepdims=True)
        odd = acc[2 * s + 1] / jnp.sum(total[2 * s + 1], axis=1, keepdims=True)
        even = pltpu.roll(even, HEAD_DIM, 1)
        out_ref[s] = jnp.where(lane < HEAD_DIM, even, odd).astype(jnp.bfloat16)
        return 0

    lax.fori_loop(0, N, finish, 0)


def attend(tab, qz, kv, far, acc, total, top):
    b16 = jnp.bfloat16
    vm = pl.BlockSpec(memory_space=pltpu.VMEM)
    state = jax.ShapeDtypeStruct(acc.shape, acc.dtype)
    return pl.pallas_call(
        attend_kernel,
        out_shape=(jax.ShapeDtypeStruct((N, TILE, TILE), b16), state, state, state),
        in_specs=[pl.BlockSpec(memory_space=pltpu.SMEM)] + [vm] * 6,
        out_specs=(vm,) * 4,
        input_output_aliases={4: 1, 5: 2, 6: 3},
        scratch_shapes=[
            pltpu.VMEM((GROUP + N * SLOTS, TILE, TILE), b16),
            pltpu.SMEM((GROUP + 1,), jnp.int32),
            *scratch_state(),
        ],
        compiler_params=pltpu.CompilerParams(vmem_limit_bytes=24 << 20),
        name="attend",
    )(tab, qz, kv, far, acc, total, top)[0]


def finish_kernel(att_ref, nodes_ref, w_ref, out_ref, got, joined, ss, rs):
    me = lax.axis_index("sp")
    barrier = pltpu.get_barrier_semaphore()

    def greet(d, _):
        pl.semaphore_signal(barrier, inc=1, device_id={"sp": lax.rem(me + d, N)}, device_id_type=MESH)
        return 0

    lax.fori_loop(1, N, greet, 0)
    pl.semaphore_wait(barrier, N - 1)

    def copy(dst, idx):
        return pltpu.make_async_remote_copy(
            src_ref=att_ref.at[dst], dst_ref=got.at[idx], send_sem=ss.at[dst],
            recv_sem=rs.at[idx], device_id={"sp": dst}, device_id_type=MESH)

    def send(d, _):
        copy(lax.rem(me + d, N), me).start()
        return 0

    lax.fori_loop(1, N, send, 0)
    got[me] = att_ref[me]

    def drain(d, _):
        s = lax.rem(me + N - d, N)
        copy(s, s).wait_recv()
        copy(s, s).wait_send()
        return 0

    lax.fori_loop(1, N, drain, 0)
    for p in range(HEADS // 2):
        a, b = got[2 * p], got[2 * p + 1]
        cols = slice(p * TILE, (p + 1) * TILE)
        joined[:TILE, cols] = jnp.concatenate([a[:, :HEAD_DIM], b[:, :HEAD_DIM]], axis=1)
        joined[TILE:, cols] = jnp.concatenate([a[:, HEAD_DIM:], b[:, HEAD_DIM:]], axis=1)
    for c in range(4):
        cols = slice(c * 256, (c + 1) * 256)
        y = jnp.dot(joined[...], w_ref[:, cols], preferred_element_type=jnp.float32)
        out_ref[:, cols] = (nodes_ref[:, cols].astype(jnp.float32) + y).astype(jnp.bfloat16)


def finish(att, nodes, project_out):
    b16 = jnp.bfloat16
    vm = pl.BlockSpec(memory_space=pltpu.VMEM)
    dma = pltpu.SemaphoreType.DMA
    return pl.pallas_call(
        finish_kernel,
        out_shape=jax.ShapeDtypeStruct((2 * TILE, D), b16),
        in_specs=[vm, vm, vm],
        out_specs=vm,
        scratch_shapes=[
            pltpu.VMEM((N, TILE, TILE), b16),
            pltpu.VMEM((2 * TILE, D), b16),
            dma((N,)), dma((N,)),
        ],
        compiler_params=pltpu.CompilerParams(
            collective_id=1, has_side_effects=True, vmem_limit_bytes=24 << 20),
        name="finish",
    )(att, nodes, project_out)


def shards(nodes, project_in, project_out, tile_list, tile_count):
    arguments = (tile_list.T, tile_count[None, :], nodes, project_in)
    arguments = [pltpu.with_memory_space_constraint(a, pltpu.HBM) for a in arguments]
    qz, kv, far, tab, acc, total, top = exchange(*arguments)
    att = attend(tab, qz, kv, far, acc, total, top)
    return finish(att, nodes, project_out)


def solution(mesh):
    in_specs = (P(("pb", "sp"), None), P(), P(), P(), P())
    out_specs = P(("pb", "sp"), None)
    return jax.shard_map(shards, mesh=mesh, in_specs=in_specs, out_specs=out_specs, check_vma=False)
```

```python
import functools

import jax
import jax.numpy as jnp
from jax import lax
from jax.experimental import pallas as pl
from jax.experimental.pallas import tpu as pltpu
from jax.sharding import PartitionSpec as P

D = 1024
HEADS = 16
HEAD_DIM = 64
TILE = 128
LISTED = 32
SLOTS = 4
GROUP = 32
N = 16
CHUNK = 4
EARLY = 8
HALF = GROUP // 2
RAW = 2
PART = TILE // N
LOW = -1e30
MESH = pl.DeviceIdType.MESH


def build_tables(list_ref, count_ref, marked_ref, tab_ref, grp):
    f32, b16, i32 = jnp.float32, jnp.bfloat16, jnp.int32
    base = grp * GROUP
    places = lax.broadcasted_iota(i32, (LISTED, N * GROUP), 0)
    across = jnp.where(places < count_ref[...], list_ref[...], -1)
    for b in range(0, N * GROUP, TILE):
        marked_ref[b:b + TILE, :] = across[:, b:b + TILE].T
    lane = lax.broadcasted_iota(i32, (N, TILE), 1)

    def uses(i, used):
        hit = jnp.where(marked_ref[...] == base + i, 1.0, 0.0)
        hit = jnp.max(hit.reshape(N, GROUP, LISTED), axis=1)
        return jnp.where(lane == i, jnp.max(hit, axis=1, keepdims=True), used)

    used = lax.fori_loop(0, GROUP, uses, jnp.zeros((N, TILE), f32), unroll=4)
    low = lax.broadcasted_iota(i32, (TILE, TILE), 0) < lax.broadcasted_iota(i32, (TILE, TILE), 1)
    rank = jnp.dot(used.astype(b16), jnp.where(low, 1.0, 0.0).astype(b16), preferred_element_type=f32)
    send = jnp.zeros((N, TILE), f32)
    for k in range(SLOTS):
        pick = jnp.where((rank == k) & (used > 0), lane.astype(f32), 0.0)
        send = jnp.where(lane == k, jnp.sum(pick, axis=1, keepdims=True), send)
    tab_ref[GROUP:] = send.astype(i32)
    tiles = N * GROUP
    own = marked_ref[pl.ds(pl.multiple_of(base, GROUP), GROUP), :]
    tile = lax.broadcasted_iota(i32, (GROUP, tiles), 1)
    present = jnp.zeros((GROUP, tiles), f32)
    for j in range(LISTED):
        present = jnp.where(own[:, j:j + 1] == tile, 1.0, present)
    up = lax.broadcasted_iota(i32, (tiles, tiles), 0)
    across = lax.broadcasted_iota(i32, (tiles, tiles), 1)
    before = up < across
    same = before & (lax.div(up, GROUP) == lax.div(across, GROUP))
    before = jnp.where(before, 1.0, 0.0).astype(b16)
    same = jnp.where(same, 1.0, 0.0).astype(b16)
    wanted = jnp.broadcast_to(jnp.max(present, axis=0, keepdims=True), (N, tiles))
    rank = jnp.dot(wanted.astype(b16), same, preferred_element_type=f32)[0:1]
    owner = lax.div(tile, GROUP)
    here = owner == grp
    raw = (GROUP + RAW * owner).astype(f32) + rank
    cooked = (GROUP + RAW * N - RAW + (SLOTS - RAW) * owner).astype(f32) + rank
    slot = jnp.where(here, (tile - base).astype(f32), jnp.where(rank < RAW, raw, cooked))
    near = jnp.where(here, present, 0.0)
    away = jnp.where(here, 0.0, present)
    both = jnp.concatenate([near, away], axis=0).astype(b16)
    order = jnp.dot(both, before, preferred_element_type=f32)
    near_count = jnp.sum(near, axis=1, keepdims=True)
    count = jnp.sum(present, axis=1, keepdims=True)
    order = jnp.where(here, order[:GROUP], order[GROUP:] + near_count)
    order = jnp.where(present > 0, order, -1.0)
    wide = lax.broadcasted_iota(i32, (GROUP, TILE), 1)

    def place(k, out):
        v = jnp.sum(jnp.where(order == k.astype(f32), slot, 0.0), axis=1, keepdims=True)
        return jnp.where(wide == k, v, out)

    out = lax.fori_loop(0, LISTED, place, jnp.zeros((GROUP, TILE), f32), unroll=4)
    out = jnp.where(wide == LISTED, near_count, out)
    out = jnp.where(wide == LISTED + 1, count, out)
    tab_ref[:GROUP] = out.astype(i32)


def scratch_state():
    f32 = jnp.float32
    square = pltpu.VMEM((TILE, TILE), f32)
    return 2 * [
        pltpu.VMEM((2, TILE, CHUNK * TILE), f32),
        pltpu.VMEM((TILE, CHUNK * TILE), jnp.bfloat16),
        square, square, square, square,
    ]


def clear_stages(buffers):
    for ref in buffers:
        ref[...] = jnp.zeros_like(ref)


def run_stages(slot, items, fetch, live, qz, base, state, buffers):
    acc, total, top = state
    s_buf, p_buf, m_cur, m_max, a_cur, a_old = buffers
    (r0, c0), (r1, _), (r2, _), (r3, c3) = items
    added = jnp.dot(p_buf[...], fetch(r3, c3), preferred_element_type=jnp.float32)
    acc[r3] = acc[r3] * a_old[...] + added
    m = m_cur[...]
    fade = a_cur[...]
    part = None
    for t in range(CHUNK):
        cols = slice(t * TILE, (t + 1) * TILE)
        w = jnp.exp(s_buf[slot, :, cols] - m)
        p_buf[:, cols] = w.astype(jnp.bfloat16)
        part = w if part is None else part + w
    total[r2] = total[r2] * fade + part
    a_old[...] = fade
    before = top[r1]
    now = jnp.maximum(before, jnp.max(m_max[...], axis=1, keepdims=True))
    top[r1] = now
    m_cur[...] = now
    a_cur[...] = jnp.exp(before - now)
    row = jnp.minimum(r0, HALF - 1) + base
    s = lax.dot_general(
        qz[row], fetch(r0, c0), (((1,), (1,)), ((), ())), preferred_element_type=jnp.float32)
    big = None
    for t in range(CHUNK):
        cols = slice(t * TILE, (t + 1) * TILE)
        st = s[:, cols] + jnp.where(c0 + t < live(row), 0.0, LOW)
        s_buf[slot, :, cols] = st
        big = st if big is None else jnp.maximum(big, st)
    m_max[...] = big


def exchange_kernel(
    list_hbm, count_hbm, nodes_hbm, parts_hbm, w_hbm,
    qz, kv_out, raw_out, far_out, tab_out, acc_a, total_a, top_a, acc_b, total_b, top_b,
    w_buf, kv_send, q_send, q_got, far_send, parts, part_got, part_send, part_far, raw_send, raw_got,
    list_ref, count_ref, nodes_ref, marked, tab, in_sem, w_sem, kv_ss, kv_rs, q_ss, q_rs, z_ss, z_rs,
    p_ss, p_rs, y_ss, y_rs, r_ss, r_rs, t_sem,
    *buffers,
):
    me = lax.axis_index("sp")
    grp = lax.axis_index("pb")

    def w_copy(p):
        cols = pl.ds(pl.multiple_of(p * 384, 128), 384)
        return pltpu.make_async_copy(w_hbm.at[:, cols], w_buf.at[p], w_sem.at[p])

    def pair(i):
        return lax.rem(me // 2 + i, 8)

    arrivals = [
        pltpu.make_async_copy(a, b, in_sem.at[i])
        for i, (a, b) in enumerate((
            (parts_hbm, parts), (nodes_hbm, nodes_ref), (list_hbm, list_ref), (count_hbm, count_ref)))
    ]
    for copy in arrivals:
        copy.start()
    for i in range(8):
        w_copy(pair(i)).start()

    barrier = pltpu.get_barrier_semaphore()

    def greet(d, _):
        pl.semaphore_signal(barrier, inc=1, device_id={"sp": lax.rem(me + d, N)}, device_id_type=MESH)
        pl.semaphore_signal(barrier, inc=1, device_id={"pb": lax.rem(grp + d, N)}, device_id_type=MESH)
        return 0

    lax.fori_loop(1, N, greet, 0)
    pl.semaphore_wait(barrier, 2 * (N - 1))

    def kv_copy(src, dst, idx):
        return pltpu.make_async_remote_copy(
            src_ref=kv_send.at[dst], dst_ref=kv_out.at[pl.ds(2 * idx, 2)], send_sem=kv_ss.at[dst],
            recv_sem=kv_rs.at[idx], device_id={"sp": dst}, device_id_type=MESH)

    def q_copy(dst, idx):
        return pltpu.make_async_remote_copy(
            src_ref=q_send.at[dst], dst_ref=q_got.at[idx], send_sem=q_ss.at[dst],
            recv_sem=q_rs.at[idx], device_id={"sp": dst}, device_id_type=MESH)

    def project(i, _):
        p = pair(i)
        w_copy(p).wait()
        y = jnp.dot(nodes_ref[...], w_buf[p], preferred_element_type=jnp.float32)
        for k in range(2):
            h = 2 * p + k
            o = k * 192
            q = (y[:, o:o + 64] * HEAD_DIM ** -0.5).astype(jnp.bfloat16)
            kv_send[h] = y[:, o + 64:o + 192].astype(jnp.bfloat16).reshape(2, TILE, TILE)
            q_send[h] = jnp.concatenate([q[:TILE], q[TILE:]], axis=1)

            @pl.when(h != me)
            def _():
                kv_copy(me, h, me).start()
        return 0

    def part_copy(dst, idx):
        return pltpu.make_async_remote_copy(
            src_ref=parts.at[:, dst], dst_ref=part_got.at[pl.ds(2 * idx, 2)], send_sem=p_ss.at[dst],
            recv_sem=p_rs.at[idx], device_id={"sp": dst}, device_id_type=MESH)

    def send_part(d, _):
        part_copy(lax.rem(me + d, N), me).start()
        return 0

    arrivals[0].wait()
    lax.fori_loop(1, N, send_part, 0)
    own_part = pltpu.make_async_copy(parts.at[:, me], part_got.at[pl.ds(2 * me, 2)], in_sem.at[0])
    own_part.start()
    for copy in arrivals[1:]:
        copy.wait()
    lax.fori_loop(0, 8, project, 0)
    own_part.wait()
    kv_out[pl.ds(2 * me, 2)] = kv_send[me]
    q_got[me] = q_send[me]

    def send_q(d, _):
        q_copy(lax.rem(me + d, N), me).start()
        return 0

    lax.fori_loop(1, N, send_q, 0)

    build_tables(list_ref, count_ref, marked, tab_out, grp)
    to_scalar = pltpu.make_async_copy(tab_out, tab, t_sem)
    to_scalar.start()

    states = ((acc_a, total_a, top_a), (acc_b, total_b, top_b))

    def clear(r, _):
        for acc, total, top in states:
            acc[r] = jnp.zeros((TILE, TILE), jnp.float32)
            total[r] = jnp.zeros((TILE, TILE), jnp.float32)
            top[r] = jnp.full((TILE, TILE), LOW, jnp.float32)
        return 0

    lax.fori_loop(0, HALF + 1, clear, 0)
    clear_stages(buffers)
    to_scalar.wait()

    def off_of(d):
        half = lax.div(d + 1, 2)
        return 8 + half * (2 * lax.rem(d, 2) - 1)

    def part_wait(d, _):
        s = lax.rem(me + N - d, N)
        part_copy(s, s).wait_recv()
        return 0

    lax.fori_loop(1, N, part_wait, 0)

    def wanted(dst, k):
        return jnp.clip(tab[GROUP + dst, k], 0, GROUP - 1)

    def far_part(dst, idx):
        return pltpu.make_async_remote_copy(
            src_ref=part_send.at[dst], dst_ref=part_far.at[idx], send_sem=y_ss.at[dst],
            recv_sem=y_rs.at[idx], device_id={"pb": dst}, device_id_type=MESH)

    def select_part(d, _):
        dst = lax.rem(grp + off_of(d), N)
        rows = [part_got[wanted(dst, k)].astype(jnp.float32) for k in range(RAW)]
        part_send[dst] = jnp.concatenate(rows, axis=0).astype(jnp.bfloat16)
        far_part(dst, grp).start()
        return 0

    lax.fori_loop(0, N - 1, select_part, 0)
    part_far[grp] = jnp.zeros((RAW * PART, D), jnp.bfloat16)

    def wait_kv(d, _):
        s = lax.rem(me + N - d, N)
        kv_copy(me, s, s).wait_recv()
        return 0

    lax.fori_loop(1, N, wait_kv, 0)

    def far_copy(dst, idx):
        return pltpu.make_async_remote_copy(
            src_ref=far_send.at[dst], dst_ref=far_out.at[pl.ds((SLOTS - RAW) * idx, SLOTS - RAW)], send_sem=z_ss.at[dst],
            recv_sem=z_rs.at[idx], device_id={"pb": dst}, device_id_type=MESH)

    def select(d, _):
        dst = lax.rem(grp + off_of(d), N)
        for k in range(RAW, SLOTS):
            far_send[dst, k - RAW] = kv_out[wanted(dst, k)]
        far_copy(dst, grp).start()
        return 0

    lax.fori_loop(0, N - 1, select, 0)
    far_out[pl.ds((SLOTS - RAW) * grp, SLOTS - RAW)] = kv_out[0:SLOTS - RAW]

    def part_arrive(d, _):
        s = lax.rem(grp + N - d, N)
        far_part(s, s).wait_recv()
        return 0

    lax.fori_loop(1, N, part_arrive, 0)

    def raw_copy(dst, idx):
        return pltpu.make_async_remote_copy(
            src_ref=raw_send.at[dst], dst_ref=raw_got.at[idx], send_sem=r_ss.at[dst],
            recv_sem=r_rs.at[idx], device_id={"sp": dst}, device_id_type=MESH)

    def project_raw(i, _):
        p = pair(i)
        x = part_far[...].reshape(N * RAW * PART, D)
        y = jnp.dot(x, w_buf[p], preferred_element_type=jnp.float32)
        for k in range(2):
            h = 2 * p + k
            o = k * 192
            raw_send[h] = y[:, o + 64:o + 192].astype(jnp.bfloat16)

            @pl.when(h != me)
            def _():
                raw_copy(h, me).start()
        return 0

    lax.fori_loop(0, 8, project_raw, 0)
    raw_got[me] = raw_send[me]

    def drain(d, _):
        s = lax.rem(me + N - d, N)
        q_copy(s, s).wait_recv()
        q_copy(s, s).wait_send()
        kv_copy(me, s, s).wait_send()
        part_copy(s, s).wait_send()
        return 0

    lax.fori_loop(1, N, drain, 0)
    zero64 = jnp.zeros((TILE, HEAD_DIM), jnp.bfloat16)

    def setup(s, _):
        both = q_got[s]
        qz[2 * s] = jnp.concatenate([both[:, :HEAD_DIM], zero64], axis=1)
        qz[2 * s + 1] = jnp.concatenate([both[:, HEAD_DIM:], zero64], axis=1)
        return 0

    lax.fori_loop(0, N, setup, 0)

    def fetch_from(base):
        def fetch(r, c):
            row = jnp.minimum(r, HALF - 1) + base
            return jnp.concatenate(
                [kv_out[jnp.clip(tab[row, c + t], 0, GROUP - 1)] for t in range(CHUNK)], axis=0)
        return fetch

    per_row = EARLY // CHUNK
    steps = HALF * per_row

    def item(i):
        valid = (i >= 0) & (i < steps)
        i = jnp.clip(i, 0, steps - 1)
        row = lax.div(i, per_row)
        return jnp.where(valid, row, HALF), (i - row * per_row) * CHUNK

    def advance(i, _):
        items = [item(i - k) for k in range(4)]
        for k in range(2):
            run_stages(
                lax.rem(i, 2), items, fetch_from(k * HALF), lambda row: tab[row, LISTED], qz,
                k * HALF, states[k], buffers[6 * k:6 * k + 6])
        return 0

    lax.fori_loop(0, steps + 3, advance, 0)

    def drain_raw(d, _):
        s = lax.rem(me + N - d, N)
        raw_copy(s, s).wait_recv()
        raw_copy(s, s).wait_send()
        return 0

    lax.fori_loop(1, N, drain_raw, 0)

    def assemble(o, _):
        rows = pl.ds(pl.multiple_of(o * RAW * PART, RAW * PART), RAW * PART)
        pieces = [raw_got[s, rows, :].astype(jnp.float32) for s in range(N)]
        for k in range(RAW):
            tile = jnp.concatenate([x[k * PART:(k + 1) * PART] for x in pieces], axis=0)
            raw_out[o * RAW + k] = tile.astype(jnp.bfloat16)
        return 0

    lax.fori_loop(0, N, assemble, 0)

    def drain_far(d, _):
        s = lax.rem(grp + N - d, N)
        far_part(s, s).wait_send()
        far_copy(s, s).wait_recv()
        far_copy(s, s).wait_send()
        return 0

    lax.fori_loop(1, N, drain_far, 0)


def exchange(listed, count, nodes, parts, project_in):
    b16, f32, i32 = jnp.bfloat16, jnp.float32, jnp.int32
    vm = pl.BlockSpec(memory_space=pltpu.VMEM)
    dma = pltpu.SemaphoreType.DMA
    state = jax.ShapeDtypeStruct((HALF + 1, TILE, TILE), f32)
    return pl.pallas_call(
        exchange_kernel,
        out_shape=(
            jax.ShapeDtypeStruct((GROUP, TILE, TILE), b16),
            jax.ShapeDtypeStruct((GROUP, TILE, TILE), b16),
            jax.ShapeDtypeStruct((N * RAW, TILE, TILE), b16),
            jax.ShapeDtypeStruct((N * (SLOTS - RAW), TILE, TILE), b16),
            jax.ShapeDtypeStruct((GROUP + N, TILE), i32),
            *[state] * 6,
        ),
        in_specs=[pl.BlockSpec(memory_space=pltpu.HBM)] * 5,
        out_specs=(vm,) * 11,
        scratch_shapes=[
            pltpu.VMEM((8, D, 384), b16),
            pltpu.VMEM((N, 2, TILE, TILE), b16),
            pltpu.VMEM((N, TILE, TILE), b16),
            pltpu.VMEM((N, TILE, TILE), b16),
            pltpu.VMEM((N, SLOTS - RAW, TILE, TILE), b16),
            pltpu.VMEM((2, N, PART, D), b16),
            pltpu.VMEM((GROUP, PART, D), b16),
            pltpu.VMEM((N, RAW * PART, D), b16),
            pltpu.VMEM((N, RAW * PART, D), b16),
            pltpu.VMEM((N, N * RAW * PART, TILE), b16),
            pltpu.VMEM((N, N * RAW * PART, TILE), b16),
            pltpu.VMEM((LISTED, N * GROUP), i32),
            pltpu.VMEM((1, N * GROUP), i32),
            pltpu.VMEM((2 * TILE, D), b16),
            pltpu.VMEM((N * GROUP, LISTED), i32),
            pltpu.SMEM((GROUP + N, TILE), i32),
            dma((4,)), dma((8,)), *[dma((N,))] * 12, dma,
            *scratch_state(),
        ],
        compiler_params=pltpu.CompilerParams(
            collective_id=0, has_side_effects=True, vmem_limit_bytes=30 << 20),
        name="exchange",
    )(listed, count, nodes, parts, project_in)


def attend_kernel(tab, qz, kv_ref, raw_ref, far_ref, *refs):
    out_ref, acc_a, total_a, top_a, acc_b, total_b, top_b, kv, rows = refs[6:15]
    buffers = refs[15:]
    states = ((acc_a, total_a, top_a), (acc_b, total_b, top_b))
    kv[0:GROUP] = kv_ref[...]
    kv[GROUP:GROUP + N * RAW] = raw_ref[...]
    kv[GROUP + N * RAW:] = far_ref[...]
    lane = lax.broadcasted_iota(jnp.int32, (TILE, TILE), 1)
    clear_stages(buffers)

    def first(r):
        return jnp.minimum(tab[r, LISTED], EARLY)

    used, items = [], []
    for k in range(2):
        def gather(r, carry, base=k * HALF, k=k):
            n, total = carry
            left = tab[r + base, LISTED + 1] - first(r + base)
            rows[k, n] = r
            return n + jnp.where(left > 0, 1, 0), total + lax.div(left + CHUNK - 1, CHUNK)

        n, total = lax.fori_loop(0, HALF, gather, (jnp.int32(0), jnp.int32(0)), unroll=4)
        rows[k, n] = HALF
        used.append(n)
        items.append(total)

    def fetch_from(base):
        def fetch(r, c):
            row = jnp.minimum(r, HALF - 1) + base
            return jnp.concatenate(
                [kv[tab[row, jnp.minimum(c + t, LISTED - 1)]] for t in range(CHUNK)], axis=0)
        return fetch

    def advance(i, state):
        following = []
        for k in range(2):
            n, r0, c0, r1, c1, r2, c2, r3, c3 = state[9 * k:9 * k + 9]
            base = k * HALF
            run_stages(
                lax.rem(i, 2), ((r0, c0), (r1, c1), (r2, c2), (r3, c3)), fetch_from(base),
                lambda row: tab[row, LISTED + 1], qz, base, states[k], buffers[6 * k:6 * k + 6])
            row = jnp.minimum(r0, HALF - 1) + base
            more = (c0 + CHUNK < tab[row, LISTED + 1]) & (r0 < HALF)
            n = jnp.where(more, n, jnp.minimum(n + 1, used[k]))
            rn = jnp.where(more, r0, rows[k, n])
            cn = jnp.where(more, c0 + CHUNK, first(jnp.minimum(rn, HALF - 1) + base))
            following += [n, rn, cn, r0, c0, r1, c1, r2, c2]
        return tuple(following)

    zero, dummy = jnp.int32(0), jnp.int32(HALF)
    start = []
    for k in range(2):
        r = rows[k, 0]
        start += [zero, r, first(jnp.minimum(r, HALF - 1) + k * HALF), dummy, zero, dummy, zero, dummy, zero]
    lax.fori_loop(0, jnp.maximum(items[0], items[1]) + 3, advance, tuple(start))

    def close(acc, total, r):
        return acc[r] / jnp.sum(total[r], axis=1, keepdims=True)

    def finish(s, _):
        for k, (acc, total, _top) in enumerate(states):
            even = pltpu.roll(close(acc, total, 2 * s), HEAD_DIM, 1)
            odd = close(acc, total, 2 * s + 1)
            out_ref[s + k * HALF // 2] = jnp.where(lane < HEAD_DIM, even, odd).astype(jnp.bfloat16)
        return 0

    lax.fori_loop(0, HALF // 2, finish, 0)


def attend(tab, qz, kv, raw, far, *state):
    b16 = jnp.bfloat16
    vm = pl.BlockSpec(memory_space=pltpu.VMEM)
    kept = [jax.ShapeDtypeStruct(x.shape, x.dtype) for x in state]
    return pl.pallas_call(
        attend_kernel,
        out_shape=(jax.ShapeDtypeStruct((N, TILE, TILE), b16), *kept),
        in_specs=[pl.BlockSpec(memory_space=pltpu.SMEM)] + [vm] * 10,
        out_specs=(vm,) * 7,
        input_output_aliases={5 + i: 1 + i for i in range(6)},
        scratch_shapes=[
            pltpu.VMEM((GROUP + N * SLOTS, TILE, TILE), b16),
            pltpu.SMEM((2, HALF + 1), jnp.int32),
            *scratch_state(),
        ],
        compiler_params=pltpu.CompilerParams(vmem_limit_bytes=24 << 20),
        name="attend",
    )(tab, qz, kv, raw, far, *state)[0]


def finish_kernel(att_ref, nodes_ref, w_ref, out_ref, got, joined, ss, rs):
    me = lax.axis_index("sp")
    barrier = pltpu.get_barrier_semaphore()

    def greet(d, _):
        pl.semaphore_signal(barrier, inc=1, device_id={"sp": lax.rem(me + d, N)}, device_id_type=MESH)
        return 0

    lax.fori_loop(1, N, greet, 0)
    pl.semaphore_wait(barrier, N - 1)

    def copy(dst, idx):
        return pltpu.make_async_remote_copy(
            src_ref=att_ref.at[dst], dst_ref=got.at[idx], send_sem=ss.at[dst],
            recv_sem=rs.at[idx], device_id={"sp": dst}, device_id_type=MESH)

    def send(d, _):
        copy(lax.rem(me + d, N), me).start()
        return 0

    lax.fori_loop(1, N, send, 0)
    got[me] = att_ref[me]

    def drain(d, _):
        s = lax.rem(me + N - d, N)
        copy(s, s).wait_recv()
        copy(s, s).wait_send()
        return 0

    lax.fori_loop(1, N, drain, 0)
    for p in range(HEADS // 2):
        a, b = got[2 * p], got[2 * p + 1]
        cols = slice(p * TILE, (p + 1) * TILE)
        joined[:TILE, cols] = jnp.concatenate([a[:, :HEAD_DIM], b[:, :HEAD_DIM]], axis=1)
        joined[TILE:, cols] = jnp.concatenate([a[:, HEAD_DIM:], b[:, HEAD_DIM:]], axis=1)
    for c in range(4):
        cols = slice(c * 256, (c + 1) * 256)
        y = jnp.dot(joined[...], w_ref[:, cols], preferred_element_type=jnp.float32)
        out_ref[:, cols] = (nodes_ref[:, cols].astype(jnp.float32) + y).astype(jnp.bfloat16)


def finish(att, nodes, project_out):
    b16 = jnp.bfloat16
    vm = pl.BlockSpec(memory_space=pltpu.VMEM)
    dma = pltpu.SemaphoreType.DMA
    return pl.pallas_call(
        finish_kernel,
        out_shape=jax.ShapeDtypeStruct((2 * TILE, D), b16),
        in_specs=[vm, vm, vm],
        out_specs=vm,
        scratch_shapes=[
            pltpu.VMEM((N, TILE, TILE), b16),
            pltpu.VMEM((2 * TILE, D), b16),
            dma((N,)), dma((N,)),
        ],
        compiler_params=pltpu.CompilerParams(
            collective_id=1, has_side_effects=True, vmem_limit_bytes=24 << 20),
        name="finish",
    )(att, nodes, project_out)


def shards(nodes, project_in, project_out, tile_list, tile_count):
    arguments = (
        tile_list.T, tile_count[None, :], nodes, nodes.reshape(2, N, PART, D), project_in)
    arguments = [pltpu.with_memory_space_constraint(a, pltpu.HBM) for a in arguments]
    qz, kv, raw, far, tab, *state = exchange(*arguments)
    att = attend(tab, qz, kv, raw, far, *state)
    return finish(att, nodes, project_out)


def solution(mesh):
    in_specs = (P(("pb", "sp"), None), P(), P(), P(), P())
    out_specs = P(("pb", "sp"), None)
    return jax.shard_map(shards, mesh=mesh, in_specs=in_specs, out_specs=out_specs, check_vma=False)
```

```python
import functools

import jax
import jax.numpy as jnp
from jax import lax
from jax.experimental import pallas as pl
from jax.experimental.pallas import tpu as pltpu
from jax.sharding import PartitionSpec as P

D = 1024
HEADS = 16
HEAD_DIM = 64
TILE = 128
LISTED = 32
SLOTS = 4
GROUP = 32
N = 16
CHUNK = 4
EARLY = 8
HALF = GROUP // 2
RAW = 2
PART = TILE // N
LOW = -1e30
MESH = pl.DeviceIdType.MESH


def list_sends(list_ref, count_ref, live_ref, used_ref, send_ref, grp):
    f32, b16, i32 = jnp.float32, jnp.bfloat16, jnp.int32
    tiles = N * GROUP
    places = lax.broadcasted_iota(i32, (LISTED, tiles), 0)
    live_ref[...] = jnp.where(places < count_ref[...], list_ref[...], -1)

    def uses(i, _):
        hit = jnp.where(live_ref[...] == grp * GROUP + i, 1.0, 0.0)
        used_ref[pl.ds(i, 1), :] = jnp.max(hit, axis=0, keepdims=True)
        return 0

    lax.fori_loop(0, GROUP, uses, 0, unroll=8)
    row = lax.broadcasted_iota(i32, (tiles, TILE), 0)
    lane = lax.broadcasted_iota(i32, (tiles, TILE), 1)
    groups = jnp.where(lax.div(row, GROUP) == lane, 1.0, 0.0).astype(b16)
    used = jnp.dot(used_ref[...].astype(b16), groups, preferred_element_type=f32)
    used = jnp.where(used > 0, 1.0, 0.0)
    up = lax.broadcasted_iota(i32, (GROUP, GROUP), 0)
    across = lax.broadcasted_iota(i32, (GROUP, GROUP), 1)
    before = jnp.where(across < up, 1.0, 0.0).astype(b16)
    rank = jnp.dot(before, used.astype(b16), preferred_element_type=f32)
    index = lax.broadcasted_iota(i32, (GROUP, TILE), 0).astype(f32)
    for k in range(SLOTS):
        pick = jnp.where((rank == k) & (used > 0), index, 0.0)
        send_ref[k:k + 1, :] = jnp.sum(pick, axis=0, keepdims=True).astype(i32)


def build_tables(live_ref, marked_ref, tab_ref, grp):
    f32, b16, i32 = jnp.float32, jnp.bfloat16, jnp.int32
    base = grp * GROUP
    across = live_ref[...]
    for b in range(0, N * GROUP, TILE):
        marked_ref[b:b + TILE, :] = across[:, b:b + TILE].T
    tiles = N * GROUP
    own = marked_ref[pl.ds(pl.multiple_of(base, GROUP), GROUP), :]
    tile = lax.broadcasted_iota(i32, (GROUP, tiles), 1)
    present = jnp.zeros((GROUP, tiles), f32)
    for j in range(LISTED):
        present = jnp.where(own[:, j:j + 1] == tile, 1.0, present)
    up = lax.broadcasted_iota(i32, (tiles, tiles), 0)
    across = lax.broadcasted_iota(i32, (tiles, tiles), 1)
    before = up < across
    same = before & (lax.div(up, GROUP) == lax.div(across, GROUP))
    before = jnp.where(before, 1.0, 0.0).astype(b16)
    same = jnp.where(same, 1.0, 0.0).astype(b16)
    wanted = jnp.broadcast_to(jnp.max(present, axis=0, keepdims=True), (N, tiles))
    rank = jnp.dot(wanted.astype(b16), same, preferred_element_type=f32)[0:1]
    owner = lax.div(tile, GROUP)
    here = owner == grp
    raw = (GROUP + RAW * owner).astype(f32) + rank
    cooked = (GROUP + RAW * N - RAW + (SLOTS - RAW) * owner).astype(f32) + rank
    slot = jnp.where(here, (tile - base).astype(f32), jnp.where(rank < RAW, raw, cooked))
    near = jnp.where(here, present, 0.0)
    away = jnp.where(here, 0.0, present)
    both = jnp.concatenate([near, away], axis=0).astype(b16)
    order = jnp.dot(both, before, preferred_element_type=f32)
    near_count = jnp.sum(near, axis=1, keepdims=True)
    count = jnp.sum(present, axis=1, keepdims=True)
    order = jnp.where(here, order[:GROUP], order[GROUP:] + near_count)
    order = jnp.where(present > 0, order, -1.0)
    wide = lax.broadcasted_iota(i32, (GROUP, TILE), 1)

    def place(k, out):
        v = jnp.sum(jnp.where(order == k.astype(f32), slot, 0.0), axis=1, keepdims=True)
        return jnp.where(wide == k, v, out)

    out = lax.fori_loop(0, LISTED, place, jnp.zeros((GROUP, TILE), f32), unroll=4)
    out = jnp.where(wide == LISTED, near_count, out)
    out = jnp.where(wide == LISTED + 1, count, out)
    tab_ref[...] = out.astype(i32)


def scratch_state():
    f32 = jnp.float32
    square = pltpu.VMEM((TILE, TILE), f32)
    return 4 * [
        pltpu.VMEM((TILE, CHUNK * TILE), f32),
        pltpu.VMEM((TILE, CHUNK * TILE), jnp.bfloat16),
        square, square, square, square,
    ]


def clear_stages(buffers):
    for ref in buffers:
        ref[...] = jnp.zeros_like(ref)


def stream_buffers(buffers, k):
    return buffers[12 * k:12 * k + 6], buffers[12 * k + 6:12 * k + 12]


def run_stages(items, fetch, live, qz, base, state, here, there):
    acc, total, top = state
    s_buf, p_buf, m_cur, m_max, a_cur, a_old = here
    _, p_last, m_last, m_max_last, a_last, a_old_last = there
    (r0, c0), (r1, _), (r2, _), (r3, c3) = items
    added = jnp.dot(p_last[...], fetch(r3, c3), preferred_element_type=jnp.float32)
    acc[r3] = acc[r3] * a_old_last[...] + added
    m = m_last[...]
    fade = a_last[...]
    part = None
    for t in range(CHUNK):
        cols = slice(t * TILE, (t + 1) * TILE)
        w = jnp.exp(s_buf[:, cols] - m)
        p_buf[:, cols] = w.astype(jnp.bfloat16)
        part = w if part is None else part + w
    total[r2] = total[r2] * fade + part
    a_old[...] = fade
    before = top[r1]
    now = jnp.maximum(before, jnp.max(m_max_last[...], axis=1, keepdims=True))
    top[r1] = now
    m_cur[...] = now
    a_cur[...] = jnp.exp(before - now)
    row = jnp.minimum(r0, HALF - 1) + base
    s = lax.dot_general(
        qz[row], fetch(r0, c0), (((1,), (1,)), ((), ())), preferred_element_type=jnp.float32)
    big = None
    for t in range(CHUNK):
        cols = slice(t * TILE, (t + 1) * TILE)
        st = s[:, cols] + jnp.where(c0 + t < live(row), 0.0, LOW)
        s_buf[:, cols] = st
        big = st if big is None else jnp.maximum(big, st)
    m_max[...] = big


def shifted(me, d):
    return lax.rem(me // 4 + d // 4, 4) * 4 + lax.rem(lax.rem(me, 4) + lax.rem(d, 4), 4)


def exchange_kernel(
    list_hbm, count_hbm, nodes_hbm, parts_hbm, w_hbm,
    qz, kv_out, raw_out, far_out, tab_out, acc_a, total_a, top_a, acc_b, total_b, top_b,
    w_buf, kv_send, q_send, q_got, far_send, parts, part_got, part_send, part_far, raw_send, raw_got,
    list_ref, count_ref, nodes_ref, live_ref, used_ref, sends_ref, marked, sends, tab, in_sem, w_sem, kv_ss, kv_rs, q_ss, q_rs, z_ss, z_rs,
    p_ss, p_rs, y_ss, y_rs, r_ss, r_rs, t_sem, u_sem,
    *buffers,
):
    me = lax.axis_index("sp")
    grp = lax.axis_index("pb")

    def w_copy(p):
        cols = pl.ds(pl.multiple_of(p * 384, 128), 384)
        return pltpu.make_async_copy(w_hbm.at[:, cols], w_buf.at[p], w_sem.at[p])

    def pair(i):
        return lax.rem(me // 4 + i // 2, 4) * 2 + lax.rem(lax.rem(me, 4) // 2 + i, 2)

    arrivals = [
        pltpu.make_async_copy(a, b, in_sem.at[i])
        for i, (a, b) in enumerate((
            (parts_hbm, parts), (nodes_hbm, nodes_ref), (list_hbm, list_ref), (count_hbm, count_ref)))
    ]
    for copy in arrivals:
        copy.start()
    for i in range(8):
        w_copy(pair(i)).start()

    barrier = pltpu.get_barrier_semaphore()

    def greet(d, _):
        pl.semaphore_signal(barrier, inc=1, device_id={"sp": lax.rem(me + d, N)}, device_id_type=MESH)
        pl.semaphore_signal(barrier, inc=1, device_id={"pb": lax.rem(grp + d, N)}, device_id_type=MESH)
        return 0

    lax.fori_loop(1, N, greet, 0)
    arrivals[2].wait()
    arrivals[3].wait()
    list_sends(list_ref, count_ref, live_ref, used_ref, sends_ref, grp)
    sends_copy = pltpu.make_async_copy(sends_ref, sends, u_sem)
    sends_copy.start()
    pl.semaphore_wait(barrier, 2 * (N - 1))

    def kv_copy(src, dst, idx):
        return pltpu.make_async_remote_copy(
            src_ref=kv_send.at[dst], dst_ref=kv_out.at[pl.ds(2 * idx, 2)], send_sem=kv_ss.at[dst],
            recv_sem=kv_rs.at[idx], device_id={"sp": dst}, device_id_type=MESH)

    def q_copy(dst, idx):
        return pltpu.make_async_remote_copy(
            src_ref=q_send.at[dst], dst_ref=q_got.at[idx], send_sem=q_ss.at[dst],
            recv_sem=q_rs.at[idx], device_id={"sp": dst}, device_id_type=MESH)

    def project(i, _):
        p = pair(i)
        w_copy(p).wait()
        y = jnp.dot(nodes_ref[...], w_buf[p], preferred_element_type=jnp.float32)
        for k in range(2):
            h = 2 * p + k
            o = k * 192
            q = (y[:, o:o + 64] * HEAD_DIM ** -0.5).astype(jnp.bfloat16)
            kv_send[h] = y[:, o + 64:o + 192].astype(jnp.bfloat16).reshape(2, TILE, TILE)
            q_send[h] = jnp.concatenate([q[:TILE], q[TILE:]], axis=1)

            @pl.when(h != me)
            def _():
                kv_copy(me, h, me).start()
        return 0

    def part_copy(dst, idx):
        return pltpu.make_async_remote_copy(
            src_ref=parts.at[:, dst], dst_ref=part_got.at[pl.ds(2 * idx, 2)], send_sem=p_ss.at[dst],
            recv_sem=p_rs.at[idx], device_id={"sp": dst}, device_id_type=MESH)

    def send_part(d, _):
        part_copy(shifted(me, d), me).start()
        return 0

    arrivals[0].wait()
    lax.fori_loop(1, N, send_part, 0)
    own_part = pltpu.make_async_copy(parts.at[:, me], part_got.at[pl.ds(2 * me, 2)], in_sem.at[0])
    own_part.start()
    arrivals[1].wait()
    lax.fori_loop(0, 8, project, 0)
    own_part.wait()
    kv_out[pl.ds(2 * me, 2)] = kv_send[me]
    q_got[me] = q_send[me]

    def send_q(d, _):
        q_copy(shifted(me, d), me).start()
        return 0

    lax.fori_loop(1, N, send_q, 0)

    sends_copy.wait()

    def off_of(d):
        half = lax.div(d + 1, 2)
        return 8 + half * (2 * lax.rem(d, 2) - 1)

    def part_wait(d, _):
        s = lax.rem(me + N - d, N)
        part_copy(s, s).wait_recv()
        return 0

    lax.fori_loop(1, N, part_wait, 0)

    def wanted(dst, k):
        return jnp.clip(sends[k, dst], 0, GROUP - 1)

    def far_part(dst, idx):
        return pltpu.make_async_remote_copy(
            src_ref=part_send.at[dst], dst_ref=part_far.at[idx], send_sem=y_ss.at[dst],
            recv_sem=y_rs.at[idx], device_id={"pb": dst}, device_id_type=MESH)

    def select_part(d, _):
        dst = lax.rem(grp + off_of(d), N)
        rows = [part_got[wanted(dst, k)].astype(jnp.float32) for k in range(RAW)]
        part_send[dst] = jnp.concatenate(rows, axis=0).astype(jnp.bfloat16)
        far_part(dst, grp).start()
        return 0

    lax.fori_loop(0, N - 1, select_part, 0)
    part_far[grp] = jnp.zeros((RAW * PART, D), jnp.bfloat16)
    build_tables(live_ref, marked, tab_out, grp)
    to_scalar = pltpu.make_async_copy(tab_out, tab, t_sem)
    to_scalar.start()

    states = ((acc_a, total_a, top_a), (acc_b, total_b, top_b))

    def clear(r, _):
        for acc, total, top in states:
            acc[r] = jnp.zeros((TILE, TILE), jnp.float32)
            total[r] = jnp.zeros((TILE, TILE), jnp.float32)
            top[r] = jnp.full((TILE, TILE), LOW, jnp.float32)
        return 0

    lax.fori_loop(0, HALF + 1, clear, 0)
    clear_stages(buffers)
    to_scalar.wait()


    def wait_kv(d, _):
        s = lax.rem(me + N - d, N)
        kv_copy(me, s, s).wait_recv()
        return 0

    lax.fori_loop(1, N, wait_kv, 0)

    def far_copy(dst, idx):
        return pltpu.make_async_remote_copy(
            src_ref=far_send.at[dst], dst_ref=far_out.at[pl.ds((SLOTS - RAW) * idx, SLOTS - RAW)], send_sem=z_ss.at[dst],
            recv_sem=z_rs.at[idx], device_id={"pb": dst}, device_id_type=MESH)

    def select(d, _):
        dst = lax.rem(grp + off_of(d), N)
        for k in range(RAW, SLOTS):
            far_send[dst, k - RAW] = kv_out[wanted(dst, k)]
        far_copy(dst, grp).start()
        return 0

    lax.fori_loop(0, N - 1, select, 0)
    far_out[pl.ds((SLOTS - RAW) * grp, SLOTS - RAW)] = kv_out[0:SLOTS - RAW]

    def part_arrive(d, _):
        s = lax.rem(grp + N - d, N)
        far_part(s, s).wait_recv()
        return 0

    lax.fori_loop(1, N, part_arrive, 0)

    def raw_copy(dst, idx):
        return pltpu.make_async_remote_copy(
            src_ref=raw_send.at[dst], dst_ref=raw_got.at[idx], send_sem=r_ss.at[dst],
            recv_sem=r_rs.at[idx], device_id={"sp": dst}, device_id_type=MESH)

    def project_raw(i, _):
        p = pair(i)
        x = part_far[...].reshape(N * RAW * PART, D)
        y = jnp.dot(x, w_buf[p], preferred_element_type=jnp.float32)
        for k in range(2):
            h = 2 * p + k
            o = k * 192
            raw_send[h] = y[:, o + 64:o + 192].astype(jnp.bfloat16)

            @pl.when(h != me)
            def _():
                raw_copy(h, me).start()
        return 0

    lax.fori_loop(0, 8, project_raw, 0)
    raw_got[me] = raw_send[me]

    def drain(d, _):
        s = lax.rem(me + N - d, N)
        q_copy(s, s).wait_recv()
        return 0

    lax.fori_loop(1, N, drain, 0)

    zero64 = jnp.zeros((TILE, HEAD_DIM), jnp.bfloat16)

    def setup(s, _):
        both = q_got[s]
        qz[2 * s] = jnp.concatenate([both[:, :HEAD_DIM], zero64], axis=1)
        qz[2 * s + 1] = jnp.concatenate([both[:, HEAD_DIM:], zero64], axis=1)
        return 0

    lax.fori_loop(0, N, setup, 0)

    def fetch_from(base):
        def fetch(r, c):
            row = jnp.minimum(r, HALF - 1) + base
            return jnp.concatenate(
                [kv_out[jnp.clip(tab[row, c + t], 0, GROUP - 1)] for t in range(CHUNK)], axis=0)
        return fetch

    per_row = EARLY // CHUNK
    steps = HALF * per_row

    def item(i):
        valid = (i >= 0) & (i < steps)
        i = jnp.clip(i, 0, steps - 1)
        row = lax.div(i, per_row)
        return jnp.where(valid, row, HALF), (i - row * per_row) * CHUNK

    def advance(j, _):
        for odd in range(2):
            items = [item(2 * j + odd - k) for k in range(4)]
            for k in range(2):
                pair_of = stream_buffers(buffers, k)
                run_stages(
                    items, fetch_from(k * HALF), lambda row: tab[row, LISTED], qz,
                    k * HALF, states[k], pair_of[odd], pair_of[1 - odd])
        return 0

    lax.fori_loop(0, (steps + 4) // 2, advance, 0)

    def drain_raw(d, _):
        s = lax.rem(me + N - d, N)
        raw_copy(s, s).wait_recv()
        raw_copy(s, s).wait_send()
        q_copy(s, s).wait_send()
        kv_copy(me, s, s).wait_send()
        part_copy(s, s).wait_send()
        return 0

    lax.fori_loop(1, N, drain_raw, 0)

    def assemble(o, _):
        rows = pl.ds(pl.multiple_of(o * RAW * PART, RAW * PART), RAW * PART)
        pieces = [raw_got[s, rows, :].astype(jnp.float32) for s in range(N)]
        for k in range(RAW):
            tile = jnp.concatenate([x[k * PART:(k + 1) * PART] for x in pieces], axis=0)
            raw_out[o * RAW + k] = tile.astype(jnp.bfloat16)
        return 0

    lax.fori_loop(0, N, assemble, 0)

    def drain_far(d, _):
        s = lax.rem(grp + N - d, N)
        far_part(s, s).wait_send()
        far_copy(s, s).wait_recv()
        far_copy(s, s).wait_send()
        return 0

    lax.fori_loop(1, N, drain_far, 0)


def exchange(listed, count, nodes, parts, project_in):
    b16, f32, i32 = jnp.bfloat16, jnp.float32, jnp.int32
    vm = pl.BlockSpec(memory_space=pltpu.VMEM)
    dma = pltpu.SemaphoreType.DMA
    state = jax.ShapeDtypeStruct((HALF + 1, TILE, TILE), f32)
    return pl.pallas_call(
        exchange_kernel,
        out_shape=(
            jax.ShapeDtypeStruct((GROUP, TILE, TILE), b16),
            jax.ShapeDtypeStruct((GROUP, TILE, TILE), b16),
            jax.ShapeDtypeStruct((N * RAW, TILE, TILE), b16),
            jax.ShapeDtypeStruct((N * (SLOTS - RAW), TILE, TILE), b16),
            jax.ShapeDtypeStruct((GROUP, TILE), i32),
            *[state] * 6,
        ),
        in_specs=[pl.BlockSpec(memory_space=pltpu.HBM)] * 5,
        out_specs=(vm,) * 11,
        scratch_shapes=[
            pltpu.VMEM((8, D, 384), b16),
            pltpu.VMEM((N, 2, TILE, TILE), b16),
            pltpu.VMEM((N, TILE, TILE), b16),
            pltpu.VMEM((N, TILE, TILE), b16),
            pltpu.VMEM((N, SLOTS - RAW, TILE, TILE), b16),
            pltpu.VMEM((2, N, PART, D), b16),
            pltpu.VMEM((GROUP, PART, D), b16),
            pltpu.VMEM((N, RAW * PART, D), b16),
            pltpu.VMEM((N, RAW * PART, D), b16),
            pltpu.VMEM((N, N * RAW * PART, TILE), b16),
            pltpu.VMEM((N, N * RAW * PART, TILE), b16),
            pltpu.VMEM((LISTED, N * GROUP), i32),
            pltpu.VMEM((1, N * GROUP), i32),
            pltpu.VMEM((2 * TILE, D), b16),
            pltpu.VMEM((LISTED, N * GROUP), i32),
            pltpu.VMEM((GROUP, N * GROUP), f32),
            pltpu.VMEM((SLOTS, TILE), i32),
            pltpu.VMEM((N * GROUP, LISTED), i32),
            pltpu.SMEM((SLOTS, TILE), i32),
            pltpu.SMEM((GROUP, TILE), i32),
            dma((4,)), dma((8,)), *[dma((N,))] * 12, dma, dma,
            *scratch_state(),
        ],
        compiler_params=pltpu.CompilerParams(
            collective_id=0, has_side_effects=True, vmem_limit_bytes=30 << 20),
        name="exchange",
    )(listed, count, nodes, parts, project_in)


def attend_kernel(tab, qz, kv_ref, raw_ref, far_ref, *refs):
    out_ref, acc_a, total_a, top_a, acc_b, total_b, top_b, kv, rows = refs[6:15]
    buffers = refs[15:]
    states = ((acc_a, total_a, top_a), (acc_b, total_b, top_b))
    kv[0:GROUP] = kv_ref[...]
    kv[GROUP:GROUP + N * RAW] = raw_ref[...]
    kv[GROUP + N * RAW:] = far_ref[...]
    lane = lax.broadcasted_iota(jnp.int32, (TILE, TILE), 1)
    clear_stages(buffers)

    def first(r):
        return jnp.minimum(tab[r, LISTED], EARLY)

    used, items = [], []
    for k in range(2):
        def gather(r, carry, base=k * HALF, k=k):
            n, total = carry
            left = tab[r + base, LISTED + 1] - first(r + base)
            rows[k, n] = r
            return n + jnp.where(left > 0, 1, 0), total + lax.div(left + CHUNK - 1, CHUNK)

        n, total = lax.fori_loop(0, HALF, gather, (jnp.int32(0), jnp.int32(0)), unroll=4)
        rows[k, n] = HALF
        used.append(n)
        items.append(total)

    def fetch_from(base):
        def fetch(r, c):
            row = jnp.minimum(r, HALF - 1) + base
            return jnp.concatenate(
                [kv[tab[row, jnp.minimum(c + t, LISTED - 1)]] for t in range(CHUNK)], axis=0)
        return fetch

    def advance(_, state):
        state = list(state)
        for odd in range(2):
            for k in range(2):
                n, r0, c0, r1, c1, r2, c2, r3, c3 = state[9 * k:9 * k + 9]
                base = k * HALF
                pair_of = stream_buffers(buffers, k)
                run_stages(
                    ((r0, c0), (r1, c1), (r2, c2), (r3, c3)), fetch_from(base),
                    lambda row: tab[row, LISTED + 1], qz, base, states[k], pair_of[odd], pair_of[1 - odd])
                row = jnp.minimum(r0, HALF - 1) + base
                more = (c0 + CHUNK < tab[row, LISTED + 1]) & (r0 < HALF)
                n = jnp.where(more, n, jnp.minimum(n + 1, used[k]))
                rn = jnp.where(more, r0, rows[k, n])
                cn = jnp.where(more, c0 + CHUNK, first(jnp.minimum(rn, HALF - 1) + base))
                state[9 * k:9 * k + 9] = [n, rn, cn, r0, c0, r1, c1, r2, c2]
        return tuple(state)

    zero, dummy = jnp.int32(0), jnp.int32(HALF)
    start = []
    for k in range(2):
        r = rows[k, 0]
        start += [zero, r, first(jnp.minimum(r, HALF - 1) + k * HALF), dummy, zero, dummy, zero, dummy, zero]
    lax.fori_loop(0, lax.div(jnp.maximum(items[0], items[1]) + 4, 2), advance, tuple(start))

    def close(acc, total, r):
        return acc[r] / jnp.sum(total[r], axis=1, keepdims=True)

    def finish(s, _):
        for k, (acc, total, _top) in enumerate(states):
            even = pltpu.roll(close(acc, total, 2 * s), HEAD_DIM, 1)
            odd = close(acc, total, 2 * s + 1)
            out_ref[s + k * HALF // 2] = jnp.where(lane < HEAD_DIM, even, odd).astype(jnp.bfloat16)
        return 0

    lax.fori_loop(0, HALF // 2, finish, 0)


def attend(tab, qz, kv, raw, far, *state):
    b16 = jnp.bfloat16
    vm = pl.BlockSpec(memory_space=pltpu.VMEM)
    kept = [jax.ShapeDtypeStruct(x.shape, x.dtype) for x in state]
    return pl.pallas_call(
        attend_kernel,
        out_shape=(jax.ShapeDtypeStruct((N, TILE, TILE), b16), *kept),
        in_specs=[pl.BlockSpec(memory_space=pltpu.SMEM)] + [vm] * 10,
        out_specs=(vm,) * 7,
        input_output_aliases={5 + i: 1 + i for i in range(6)},
        scratch_shapes=[
            pltpu.VMEM((GROUP + N * SLOTS, TILE, TILE), b16),
            pltpu.SMEM((2, HALF + 1), jnp.int32),
            *scratch_state(),
        ],
        compiler_params=pltpu.CompilerParams(vmem_limit_bytes=24 << 20),
        name="attend",
    )(tab, qz, kv, raw, far, *state)[0]


def finish_kernel(att_ref, nodes_ref, w_ref, out_ref, got, joined, ss, rs):
    me = lax.axis_index("sp")
    barrier = pltpu.get_barrier_semaphore()

    def greet(d, _):
        pl.semaphore_signal(barrier, inc=1, device_id={"sp": lax.rem(me + d, N)}, device_id_type=MESH)
        return 0

    lax.fori_loop(1, N, greet, 0)
    pl.semaphore_wait(barrier, N - 1)

    def copy(dst, idx):
        return pltpu.make_async_remote_copy(
            src_ref=att_ref.at[dst], dst_ref=got.at[idx], send_sem=ss.at[dst],
            recv_sem=rs.at[idx], device_id={"sp": dst}, device_id_type=MESH)

    def send(d, _):
        copy(lax.rem(me + d, N), me).start()
        return 0

    lax.fori_loop(1, N, send, 0)
    got[me] = att_ref[me]

    def drain(d, _):
        s = lax.rem(me + N - d, N)
        copy(s, s).wait_recv()
        copy(s, s).wait_send()
        return 0

    lax.fori_loop(1, N, drain, 0)
    for p in range(HEADS // 2):
        a, b = got[2 * p], got[2 * p + 1]
        cols = slice(p * TILE, (p + 1) * TILE)
        joined[:TILE, cols] = jnp.concatenate([a[:, :HEAD_DIM], b[:, :HEAD_DIM]], axis=1)
        joined[TILE:, cols] = jnp.concatenate([a[:, HEAD_DIM:], b[:, HEAD_DIM:]], axis=1)
    for c in range(4):
        cols = slice(c * 256, (c + 1) * 256)
        y = jnp.dot(joined[...], w_ref[:, cols], preferred_element_type=jnp.float32)
        out_ref[:, cols] = (nodes_ref[:, cols].astype(jnp.float32) + y).astype(jnp.bfloat16)


def finish(att, nodes, project_out):
    b16 = jnp.bfloat16
    vm = pl.BlockSpec(memory_space=pltpu.VMEM)
    dma = pltpu.SemaphoreType.DMA
    return pl.pallas_call(
        finish_kernel,
        out_shape=jax.ShapeDtypeStruct((2 * TILE, D), b16),
        in_specs=[vm, vm, vm],
        out_specs=vm,
        scratch_shapes=[
            pltpu.VMEM((N, TILE, TILE), b16),
            pltpu.VMEM((2 * TILE, D), b16),
            dma((N,)), dma((N,)),
        ],
        compiler_params=pltpu.CompilerParams(
            collective_id=1, has_side_effects=True, vmem_limit_bytes=24 << 20),
        name="finish",
    )(att, nodes, project_out)


def shards(nodes, project_in, project_out, tile_list, tile_count):
    arguments = (
        tile_list.T, tile_count[None, :], nodes, nodes.reshape(2, N, PART, D), project_in)
    arguments = [pltpu.with_memory_space_constraint(a, pltpu.HBM) for a in arguments]
    qz, kv, raw, far, tab, *state = exchange(*arguments)
    att = attend(tab, qz, kv, raw, far, *state)
    return finish(att, nodes, project_out)


def solution(mesh):
    in_specs = (P(("pb", "sp"), None), P(), P(), P(), P())
    out_specs = P(("pb", "sp"), None)
    return jax.shard_map(shards, mesh=mesh, in_specs=in_specs, out_specs=out_specs, check_vma=False)
```

```python
import functools

import jax
import jax.numpy as jnp
from jax import lax
from jax.experimental import pallas as pl
from jax.experimental.pallas import tpu as pltpu
from jax.sharding import PartitionSpec as P

D = 1024
HEADS = 16
HEAD_DIM = 64
TILE = 128
LISTED = 32
SLOTS = 4
GROUP = 32
N = 16
CHUNK = 4
EARLY = 8
LATE = 32
COUNTS = 64
HALF = GROUP // 2
RAW = 2
PART = TILE // N
LOW = -1e30
MESH = pl.DeviceIdType.MESH


def list_sends(list_ref, count_ref, live_ref, used_ref, send_ref, grp):
    f32, b16, i32 = jnp.float32, jnp.bfloat16, jnp.int32
    tiles = N * GROUP
    places = lax.broadcasted_iota(i32, (LISTED, tiles), 0)
    live_ref[...] = jnp.where(places < count_ref[...], list_ref[...], -1)

    def uses(i, _):
        hit = jnp.where(live_ref[...] == grp * GROUP + i, 1.0, 0.0)
        used_ref[pl.ds(i, 1), :] = jnp.max(hit, axis=0, keepdims=True)
        return 0

    lax.fori_loop(0, GROUP, uses, 0, unroll=8)
    row = lax.broadcasted_iota(i32, (tiles, TILE), 0)
    lane = lax.broadcasted_iota(i32, (tiles, TILE), 1)
    groups = jnp.where(lax.div(row, GROUP) == lane, 1.0, 0.0).astype(b16)
    used = jnp.dot(used_ref[...].astype(b16), groups, preferred_element_type=f32)
    used = jnp.where(used > 0, 1.0, 0.0)
    up = lax.broadcasted_iota(i32, (GROUP, GROUP), 0)
    across = lax.broadcasted_iota(i32, (GROUP, GROUP), 1)
    before = jnp.where(across < up, 1.0, 0.0).astype(b16)
    rank = jnp.dot(before, used.astype(b16), preferred_element_type=f32)
    index = lax.broadcasted_iota(i32, (GROUP, TILE), 0).astype(f32)
    for k in range(SLOTS):
        pick = jnp.where((rank == k) & (used > 0), index, 0.0)
        send_ref[k:k + 1, :] = jnp.sum(pick, axis=0, keepdims=True).astype(i32)


def build_tables(live_ref, marked_ref, tab_ref, grp):
    f32, b16, i32 = jnp.float32, jnp.bfloat16, jnp.int32
    base = grp * GROUP
    across = live_ref[...]
    for b in range(0, N * GROUP, TILE):
        marked_ref[b:b + TILE, :] = across[:, b:b + TILE].T
    tiles = N * GROUP
    own = marked_ref[pl.ds(pl.multiple_of(base, GROUP), GROUP), :]
    tile = lax.broadcasted_iota(i32, (GROUP, tiles), 1)
    present = jnp.zeros((GROUP, tiles), f32)
    for j in range(LISTED):
        present = jnp.where(own[:, j:j + 1] == tile, 1.0, present)
    up = lax.broadcasted_iota(i32, (tiles, tiles), 0)
    across = lax.broadcasted_iota(i32, (tiles, tiles), 1)
    before = up < across
    same = before & (lax.div(up, GROUP) == lax.div(across, GROUP))
    before = jnp.where(before, 1.0, 0.0).astype(b16)
    same = jnp.where(same, 1.0, 0.0).astype(b16)
    wanted = jnp.broadcast_to(jnp.max(present, axis=0, keepdims=True), (N, tiles))
    rank = jnp.dot(wanted.astype(b16), same, preferred_element_type=f32)[0:1]
    owner = lax.div(tile, GROUP)
    here = owner == grp
    first = (GROUP + RAW * owner).astype(f32) + rank
    second = (GROUP + RAW * N - RAW + (SLOTS - RAW) * owner).astype(f32) + rank
    slot = jnp.where(here, (tile - base).astype(f32), jnp.where(rank < RAW, first, second))
    near = jnp.where(here, present, 0.0)
    raw = jnp.where(jnp.logical_not(here) & (rank < RAW), present, 0.0)
    both = jnp.concatenate([near, raw], axis=0).astype(b16)
    order = jnp.dot(both, before, preferred_element_type=f32)
    near = jnp.where(order[:GROUP] < EARLY, near, 0.0)
    raw = jnp.where(order[GROUP:] < CHUNK, raw, 0.0)
    late = present - near - raw
    last = jnp.dot(late.astype(b16), before, preferred_element_type=f32) + LATE
    order = jnp.where(near > 0, order[:GROUP], jnp.where(raw > 0, order[GROUP:] + EARLY, last))
    order = jnp.where(present > 0, order, -1.0)
    wide = lax.broadcasted_iota(i32, (GROUP, TILE), 1)

    def place(k, out):
        v = jnp.sum(jnp.where(order == k.astype(f32), slot, 0.0), axis=1, keepdims=True)
        return jnp.where(wide == k, v, out)

    out = lax.fori_loop(0, EARLY + CHUNK, place, jnp.zeros((GROUP, TILE), f32), unroll=4)
    out = lax.fori_loop(LATE, LATE + LISTED, place, out, unroll=4)
    for i, kind in enumerate((near, raw, late)):
        out = jnp.where(wide == COUNTS + i, jnp.sum(kind, axis=1, keepdims=True), out)
    tab_ref[...] = out.astype(i32)


def scratch_state():
    f32 = jnp.float32
    square = pltpu.VMEM((TILE, TILE), f32)
    return 4 * [
        pltpu.VMEM((TILE, CHUNK * TILE), f32),
        pltpu.VMEM((TILE, CHUNK * TILE), jnp.bfloat16),
        square, square, square, square,
    ]


def clear_stages(buffers):
    for ref in buffers:
        ref[...] = jnp.zeros_like(ref)


def stream_buffers(buffers, k):
    return buffers[12 * k:12 * k + 6], buffers[12 * k + 6:12 * k + 12]


def run_stages(items, fetch, live, qz, base, state, here, there):
    acc, total, top = state
    s_buf, p_buf, m_cur, m_max, a_cur, a_old = here
    _, p_last, m_last, m_max_last, a_last, a_old_last = there
    (r0, c0), (r1, _), (r2, _), (r3, c3) = items
    added = jnp.dot(p_last[...], fetch(r3, c3), preferred_element_type=jnp.float32)
    acc[r3] = acc[r3] * a_old_last[...] + added
    m = m_last[...]
    fade = a_last[...]
    part = None
    for t in range(CHUNK):
        cols = slice(t * TILE, (t + 1) * TILE)
        w = jnp.exp(s_buf[:, cols] - m)
        p_buf[:, cols] = w.astype(jnp.bfloat16)
        part = w if part is None else part + w
    total[r2] = total[r2] * fade + part
    a_old[...] = fade
    before = top[r1]
    now = jnp.maximum(before, jnp.max(m_max_last[...], axis=1, keepdims=True))
    top[r1] = now
    m_cur[...] = now
    a_cur[...] = jnp.exp(before - now)
    row = jnp.minimum(r0, HALF - 1) + base
    s = lax.dot_general(
        qz[row], fetch(r0, c0), (((1,), (1,)), ((), ())), preferred_element_type=jnp.float32)
    big = None
    for t in range(CHUNK):
        cols = slice(t * TILE, (t + 1) * TILE)
        st = s[:, cols] + jnp.where(c0 + t < live(row), 0.0, LOW)
        s_buf[:, cols] = st
        big = st if big is None else jnp.maximum(big, st)
    m_max[...] = big


def shifted(me, d):
    return lax.rem(me // 4 + d // 4, 4) * 4 + lax.rem(lax.rem(me, 4) + lax.rem(d, 4), 4)


def exchange_kernel(
    list_hbm, count_hbm, nodes_hbm, parts_hbm, w_hbm,
    qz, kv_out, raw_out, far_out, tab_out, acc_a, total_a, top_a, acc_b, total_b, top_b,
    w_buf, kv_send, q_send, q_got, far_send, parts, part_got, part_send, part_far, raw_send, raw_got,
    list_ref, count_ref, nodes_ref, live_ref, used_ref, sends_ref, marked, sends, tab, in_sem, w_sem, kv_ss, kv_rs, q_ss, q_rs, z_ss, z_rs,
    p_ss, p_rs, y_ss, y_rs, r_ss, r_rs, t_sem, u_sem,
    *buffers,
):
    me = lax.axis_index("sp")
    grp = lax.axis_index("pb")

    def w_copy(p):
        cols = pl.ds(pl.multiple_of(p * 384, 128), 384)
        return pltpu.make_async_copy(w_hbm.at[:, cols], w_buf.at[p], w_sem.at[p])

    def pair(i):
        return lax.rem(me // 4 + i // 2, 4) * 2 + lax.rem(lax.rem(me, 4) // 2 + i, 2)

    arrivals = [
        pltpu.make_async_copy(a, b, in_sem.at[i])
        for i, (a, b) in enumerate((
            (parts_hbm, parts), (nodes_hbm, nodes_ref), (list_hbm, list_ref), (count_hbm, count_ref)))
    ]
    for copy in arrivals:
        copy.start()
    for i in range(8):
        w_copy(pair(i)).start()

    barrier = pltpu.get_barrier_semaphore()

    def greet(d, _):
        pl.semaphore_signal(barrier, inc=1, device_id={"sp": lax.rem(me + d, N)}, device_id_type=MESH)
        pl.semaphore_signal(barrier, inc=1, device_id={"pb": lax.rem(grp + d, N)}, device_id_type=MESH)
        return 0

    lax.fori_loop(1, N, greet, 0)
    arrivals[2].wait()
    arrivals[3].wait()
    list_sends(list_ref, count_ref, live_ref, used_ref, sends_ref, grp)
    sends_copy = pltpu.make_async_copy(sends_ref, sends, u_sem)
    sends_copy.start()
    pl.semaphore_wait(barrier, 2 * (N - 1))

    def kv_copy(src, dst, idx):
        return pltpu.make_async_remote_copy(
            src_ref=kv_send.at[dst], dst_ref=kv_out.at[pl.ds(2 * idx, 2)], send_sem=kv_ss.at[dst],
            recv_sem=kv_rs.at[idx], device_id={"sp": dst}, device_id_type=MESH)

    def q_copy(dst, idx):
        return pltpu.make_async_remote_copy(
            src_ref=q_send.at[dst], dst_ref=q_got.at[idx], send_sem=q_ss.at[dst],
            recv_sem=q_rs.at[idx], device_id={"sp": dst}, device_id_type=MESH)

    def project(i, _):
        p = pair(i)
        w_copy(p).wait()
        y = jnp.dot(nodes_ref[...], w_buf[p], preferred_element_type=jnp.float32)
        for k in range(2):
            h = 2 * p + k
            o = k * 192
            q = (y[:, o:o + 64] * HEAD_DIM ** -0.5).astype(jnp.bfloat16)
            kv_send[h] = y[:, o + 64:o + 192].astype(jnp.bfloat16).reshape(2, TILE, TILE)
            q_send[h] = jnp.concatenate([q[:TILE], q[TILE:]], axis=1)

            @pl.when(h != me)
            def _():
                kv_copy(me, h, me).start()
        return 0

    def part_copy(dst, idx):
        return pltpu.make_async_remote_copy(
            src_ref=parts.at[:, dst], dst_ref=part_got.at[pl.ds(2 * idx, 2)], send_sem=p_ss.at[dst],
            recv_sem=p_rs.at[idx], device_id={"sp": dst}, device_id_type=MESH)

    def send_part(d, _):
        part_copy(shifted(me, d), me).start()
        return 0

    arrivals[0].wait()
    lax.fori_loop(1, N, send_part, 0)
    own_part = pltpu.make_async_copy(parts.at[:, me], part_got.at[pl.ds(2 * me, 2)], in_sem.at[0])
    own_part.start()
    arrivals[1].wait()
    lax.fori_loop(0, 8, project, 0)
    own_part.wait()
    kv_out[pl.ds(2 * me, 2)] = kv_send[me]
    q_got[me] = q_send[me]

    def send_q(d, _):
        q_copy(shifted(me, d), me).start()
        return 0

    lax.fori_loop(1, N, send_q, 0)

    sends_copy.wait()

    def off_of(d):
        half = lax.div(d + 1, 2)
        return 8 + half * (2 * lax.rem(d, 2) - 1)

    def part_wait(d, _):
        s = lax.rem(me + N - d, N)
        part_copy(s, s).wait_recv()
        return 0

    lax.fori_loop(1, N, part_wait, 0)

    def wanted(dst, k):
        return jnp.clip(sends[k, dst], 0, GROUP - 1)

    def far_part(dst, idx):
        return pltpu.make_async_remote_copy(
            src_ref=part_send.at[dst], dst_ref=part_far.at[idx], send_sem=y_ss.at[dst],
            recv_sem=y_rs.at[idx], device_id={"pb": dst}, device_id_type=MESH)

    def select_part(d, _):
        dst = lax.rem(grp + off_of(d), N)
        rows = [part_got[wanted(dst, k)].astype(jnp.float32) for k in range(RAW)]
        part_send[dst] = jnp.concatenate(rows, axis=0).astype(jnp.bfloat16)
        far_part(dst, grp).start()
        return 0

    lax.fori_loop(0, N - 1, select_part, 0)
    part_far[grp] = jnp.zeros((RAW * PART, D), jnp.bfloat16)
    build_tables(live_ref, marked, tab_out, grp)
    to_scalar = pltpu.make_async_copy(tab_out, tab, t_sem)
    to_scalar.start()

    states = ((acc_a, total_a, top_a), (acc_b, total_b, top_b))

    def clear(r, _):
        for acc, total, top in states:
            acc[r] = jnp.zeros((TILE, TILE), jnp.float32)
            total[r] = jnp.zeros((TILE, TILE), jnp.float32)
            top[r] = jnp.full((TILE, TILE), LOW, jnp.float32)
        return 0

    lax.fori_loop(0, HALF + 1, clear, 0)
    clear_stages(buffers)
    to_scalar.wait()


    def wait_kv(d, _):
        s = lax.rem(me + N - d, N)
        kv_copy(me, s, s).wait_recv()
        return 0

    lax.fori_loop(1, N, wait_kv, 0)

    def far_copy(dst, idx):
        return pltpu.make_async_remote_copy(
            src_ref=far_send.at[dst], dst_ref=far_out.at[pl.ds((SLOTS - RAW) * idx, SLOTS - RAW)], send_sem=z_ss.at[dst],
            recv_sem=z_rs.at[idx], device_id={"pb": dst}, device_id_type=MESH)

    def select(d, _):
        dst = lax.rem(grp + off_of(d), N)
        for k in range(RAW, SLOTS):
            far_send[dst, k - RAW] = kv_out[wanted(dst, k)]
        far_copy(dst, grp).start()
        return 0

    lax.fori_loop(0, N - 1, select, 0)
    far_out[pl.ds((SLOTS - RAW) * grp, SLOTS - RAW)] = kv_out[0:SLOTS - RAW]

    def part_arrive(d, _):
        s = lax.rem(grp + N - d, N)
        far_part(s, s).wait_recv()
        return 0

    lax.fori_loop(1, N, part_arrive, 0)

    def raw_copy(dst, idx):
        return pltpu.make_async_remote_copy(
            src_ref=raw_send.at[dst], dst_ref=raw_got.at[idx], send_sem=r_ss.at[dst],
            recv_sem=r_rs.at[idx], device_id={"sp": dst}, device_id_type=MESH)

    def project_raw(i, _):
        p = pair(i)
        x = part_far[...].reshape(N * RAW * PART, D)
        y = jnp.dot(x, w_buf[p], preferred_element_type=jnp.float32)
        for k in range(2):
            h = 2 * p + k
            o = k * 192
            raw_send[h] = y[:, o + 64:o + 192].astype(jnp.bfloat16)

            @pl.when(h != me)
            def _():
                raw_copy(h, me).start()
        return 0

    lax.fori_loop(0, 8, project_raw, 0)
    raw_got[me] = raw_send[me]

    def drain(d, _):
        s = lax.rem(me + N - d, N)
        q_copy(s, s).wait_recv()
        return 0

    lax.fori_loop(1, N, drain, 0)

    zero64 = jnp.zeros((TILE, HEAD_DIM), jnp.bfloat16)

    def setup(s, _):
        both = q_got[s]
        qz[2 * s] = jnp.concatenate([both[:, :HEAD_DIM], zero64], axis=1)
        qz[2 * s + 1] = jnp.concatenate([both[:, HEAD_DIM:], zero64], axis=1)
        return 0

    lax.fori_loop(0, N, setup, 0)

    def attend_early(per_row, at, table, offset, lane):
        steps = HALF * per_row

        def fetch_from(base):
            def fetch(r, c):
                row = jnp.minimum(r, HALF - 1) + base
                last = table.shape[0] - 1
                return jnp.concatenate(
                    [table[jnp.clip(tab[row, c + t] - offset, 0, last)] for t in range(CHUNK)], axis=0)
            return fetch

        def item(i):
            valid = (i >= 0) & (i < steps)
            i = jnp.clip(i, 0, steps - 1)
            row = lax.div(i, per_row)
            return jnp.where(valid, row, HALF), at + (i - row * per_row) * CHUNK

        def advance(j, _):
            for odd in range(2):
                items = [item(2 * j + odd - k) for k in range(4)]
                for k in range(2):
                    pair_of = stream_buffers(buffers, k)
                    run_stages(
                        items, fetch_from(k * HALF), lambda row: at + tab[row, lane], qz,
                        k * HALF, states[k], pair_of[odd], pair_of[1 - odd])
            return 0

        lax.fori_loop(0, (steps + 4) // 2, advance, 0)

    attend_early(EARLY // CHUNK, 0, kv_out, 0, COUNTS)

    def arrive_raw(d, _):
        s = lax.rem(me + N - d, N)
        raw_copy(s, s).wait_recv()
        return 0

    lax.fori_loop(1, N, arrive_raw, 0)

    def assemble(o, _):
        rows = pl.ds(pl.multiple_of(o * RAW * PART, RAW * PART), RAW * PART)
        pieces = [raw_got[s, rows, :].astype(jnp.float32) for s in range(N)]
        for k in range(RAW):
            tile = jnp.concatenate([x[k * PART:(k + 1) * PART] for x in pieces], axis=0)
            raw_out[o * RAW + k] = tile.astype(jnp.bfloat16)
        return 0

    lax.fori_loop(0, N, assemble, 0)
    attend_early(1, EARLY, raw_out, GROUP, COUNTS + 1)

    def drain_near(d, _):
        s = lax.rem(me + N - d, N)
        q_copy(s, s).wait_send()
        kv_copy(me, s, s).wait_send()
        part_copy(s, s).wait_send()
        raw_copy(s, s).wait_send()
        return 0

    lax.fori_loop(1, N, drain_near, 0)

    def drain_far(d, _):
        s = lax.rem(grp + N - d, N)
        far_part(s, s).wait_send()
        far_copy(s, s).wait_recv()
        far_copy(s, s).wait_send()
        return 0

    lax.fori_loop(1, N, drain_far, 0)


def exchange(listed, count, nodes, parts, project_in):
    b16, f32, i32 = jnp.bfloat16, jnp.float32, jnp.int32
    vm = pl.BlockSpec(memory_space=pltpu.VMEM)
    dma = pltpu.SemaphoreType.DMA
    state = jax.ShapeDtypeStruct((HALF + 1, TILE, TILE), f32)
    return pl.pallas_call(
        exchange_kernel,
        out_shape=(
            jax.ShapeDtypeStruct((GROUP, TILE, TILE), b16),
            jax.ShapeDtypeStruct((GROUP, TILE, TILE), b16),
            jax.ShapeDtypeStruct((N * RAW, TILE, TILE), b16),
            jax.ShapeDtypeStruct((N * (SLOTS - RAW), TILE, TILE), b16),
            jax.ShapeDtypeStruct((GROUP, TILE), i32),
            *[state] * 6,
        ),
        in_specs=[pl.BlockSpec(memory_space=pltpu.HBM)] * 5,
        out_specs=(vm,) * 11,
        scratch_shapes=[
            pltpu.VMEM((8, D, 384), b16),
            pltpu.VMEM((N, 2, TILE, TILE), b16),
            pltpu.VMEM((N, TILE, TILE), b16),
            pltpu.VMEM((N, TILE, TILE), b16),
            pltpu.VMEM((N, SLOTS - RAW, TILE, TILE), b16),
            pltpu.VMEM((2, N, PART, D), b16),
            pltpu.VMEM((GROUP, PART, D), b16),
            pltpu.VMEM((N, RAW * PART, D), b16),
            pltpu.VMEM((N, RAW * PART, D), b16),
            pltpu.VMEM((N, N * RAW * PART, TILE), b16),
            pltpu.VMEM((N, N * RAW * PART, TILE), b16),
            pltpu.VMEM((LISTED, N * GROUP), i32),
            pltpu.VMEM((1, N * GROUP), i32),
            pltpu.VMEM((2 * TILE, D), b16),
            pltpu.VMEM((LISTED, N * GROUP), i32),
            pltpu.VMEM((GROUP, N * GROUP), f32),
            pltpu.VMEM((SLOTS, TILE), i32),
            pltpu.VMEM((N * GROUP, LISTED), i32),
            pltpu.SMEM((SLOTS, TILE), i32),
            pltpu.SMEM((GROUP, TILE), i32),
            dma((4,)), dma((8,)), *[dma((N,))] * 12, dma, dma,
            *scratch_state(),
        ],
        compiler_params=pltpu.CompilerParams(
            collective_id=0, has_side_effects=True, vmem_limit_bytes=30 << 20),
        name="exchange",
    )(listed, count, nodes, parts, project_in)


def attend_kernel(tab, qz, kv_ref, raw_ref, far_ref, *refs):
    out_ref, acc_a, total_a, top_a, acc_b, total_b, top_b, kv, rows = refs[6:15]
    buffers = refs[15:]
    states = ((acc_a, total_a, top_a), (acc_b, total_b, top_b))
    kv[0:GROUP] = kv_ref[...]
    kv[GROUP:GROUP + N * RAW] = raw_ref[...]
    kv[GROUP + N * RAW:] = far_ref[...]
    lane = lax.broadcasted_iota(jnp.int32, (TILE, TILE), 1)
    clear_stages(buffers)

    used, items = [], []
    for k in range(2):
        def gather(r, carry, base=k * HALF, k=k):
            n, total = carry
            left = tab[r + base, COUNTS + 2]
            rows[k, n] = r
            return n + jnp.where(left > 0, 1, 0), total + lax.div(left + CHUNK - 1, CHUNK)

        n, total = lax.fori_loop(0, HALF, gather, (jnp.int32(0), jnp.int32(0)), unroll=4)
        rows[k, n] = HALF
        used.append(n)
        items.append(total)

    def fetch_from(base):
        def fetch(r, c):
            row = jnp.minimum(r, HALF - 1) + base
            return jnp.concatenate(
                [kv[tab[row, jnp.minimum(c + t, LATE + LISTED - 1)]] for t in range(CHUNK)], axis=0)
        return fetch

    def advance(_, state):
        state = list(state)
        for odd in range(2):
            for k in range(2):
                n, r0, c0, r1, c1, r2, c2, r3, c3 = state[9 * k:9 * k + 9]
                base = k * HALF
                pair_of = stream_buffers(buffers, k)
                run_stages(
                    ((r0, c0), (r1, c1), (r2, c2), (r3, c3)), fetch_from(base),
                    lambda row: LATE + tab[row, COUNTS + 2], qz, base, states[k], pair_of[odd], pair_of[1 - odd])
                row = jnp.minimum(r0, HALF - 1) + base
                more = (c0 + CHUNK < LATE + tab[row, COUNTS + 2]) & (r0 < HALF)
                n = jnp.where(more, n, jnp.minimum(n + 1, used[k]))
                rn = jnp.where(more, r0, rows[k, n])
                cn = jnp.where(more, c0 + CHUNK, LATE)
                state[9 * k:9 * k + 9] = [n, rn, cn, r0, c0, r1, c1, r2, c2]
        return tuple(state)

    zero, dummy, at = jnp.int32(0), jnp.int32(HALF), jnp.int32(LATE)
    start = []
    for k in range(2):
        start += [zero, rows[k, 0], at, dummy, at, dummy, at, dummy, at]
    lax.fori_loop(0, lax.div(jnp.maximum(items[0], items[1]) + 4, 2), advance, tuple(start))

    def close(acc, total, r):
        return acc[r] / jnp.sum(total[r], axis=1, keepdims=True)

    def finish(s, _):
        for k, (acc, total, _top) in enumerate(states):
            even = pltpu.roll(close(acc, total, 2 * s), HEAD_DIM, 1)
            odd = close(acc, total, 2 * s + 1)
            out_ref[s + k * HALF // 2] = jnp.where(lane < HEAD_DIM, even, odd).astype(jnp.bfloat16)
        return 0

    lax.fori_loop(0, HALF // 2, finish, 0)


def attend(tab, qz, kv, raw, far, *state):
    b16 = jnp.bfloat16
    vm = pl.BlockSpec(memory_space=pltpu.VMEM)
    kept = [jax.ShapeDtypeStruct(x.shape, x.dtype) for x in state]
    return pl.pallas_call(
        attend_kernel,
        out_shape=(jax.ShapeDtypeStruct((N, TILE, TILE), b16), *kept),
        in_specs=[pl.BlockSpec(memory_space=pltpu.SMEM)] + [vm] * 10,
        out_specs=(vm,) * 7,
        input_output_aliases={5 + i: 1 + i for i in range(6)},
        scratch_shapes=[
            pltpu.VMEM((GROUP + N * SLOTS, TILE, TILE), b16),
            pltpu.SMEM((2, HALF + 1), jnp.int32),
            *scratch_state(),
        ],
        compiler_params=pltpu.CompilerParams(vmem_limit_bytes=24 << 20),
        name="attend",
    )(tab, qz, kv, raw, far, *state)[0]


def finish_kernel(att_ref, nodes_ref, w_ref, out_ref, got, joined, ss, rs):
    me = lax.axis_index("sp")
    barrier = pltpu.get_barrier_semaphore()

    def greet(d, _):
        pl.semaphore_signal(barrier, inc=1, device_id={"sp": lax.rem(me + d, N)}, device_id_type=MESH)
        return 0

    lax.fori_loop(1, N, greet, 0)
    pl.semaphore_wait(barrier, N - 1)

    def copy(dst, idx):
        return pltpu.make_async_remote_copy(
            src_ref=att_ref.at[dst], dst_ref=got.at[idx], send_sem=ss.at[dst],
            recv_sem=rs.at[idx], device_id={"sp": dst}, device_id_type=MESH)

    def send(d, _):
        copy(lax.rem(me + d, N), me).start()
        return 0

    lax.fori_loop(1, N, send, 0)
    got[me] = att_ref[me]

    def drain(d, _):
        s = lax.rem(me + N - d, N)
        copy(s, s).wait_recv()
        copy(s, s).wait_send()
        return 0

    lax.fori_loop(1, N, drain, 0)
    for p in range(HEADS // 2):
        a, b = got[2 * p], got[2 * p + 1]
        cols = slice(p * TILE, (p + 1) * TILE)
        joined[:TILE, cols] = jnp.concatenate([a[:, :HEAD_DIM], b[:, :HEAD_DIM]], axis=1)
        joined[TILE:, cols] = jnp.concatenate([a[:, HEAD_DIM:], b[:, HEAD_DIM:]], axis=1)
    for c in range(4):
        cols = slice(c * 256, (c + 1) * 256)
        y = jnp.dot(joined[...], w_ref[:, cols], preferred_element_type=jnp.float32)
        out_ref[:, cols] = (nodes_ref[:, cols].astype(jnp.float32) + y).astype(jnp.bfloat16)


def finish(att, nodes, project_out):
    b16 = jnp.bfloat16
    vm = pl.BlockSpec(memory_space=pltpu.VMEM)
    dma = pltpu.SemaphoreType.DMA
    return pl.pallas_call(
        finish_kernel,
        out_shape=jax.ShapeDtypeStruct((2 * TILE, D), b16),
        in_specs=[vm, vm, vm],
        out_specs=vm,
        scratch_shapes=[
            pltpu.VMEM((N, TILE, TILE), b16),
            pltpu.VMEM((2 * TILE, D), b16),
            dma((N,)), dma((N,)),
        ],
        compiler_params=pltpu.CompilerParams(
            collective_id=1, has_side_effects=True, vmem_limit_bytes=24 << 20),
        name="finish",
    )(att, nodes, project_out)


def shards(nodes, project_in, project_out, tile_list, tile_count):
    arguments = (
        tile_list.T, tile_count[None, :], nodes, nodes.reshape(2, N, PART, D), project_in)
    arguments = [pltpu.with_memory_space_constraint(a, pltpu.HBM) for a in arguments]
    qz, kv, raw, far, tab, *state = exchange(*arguments)
    att = attend(tab, qz, kv, raw, far, *state)
    return finish(att, nodes, project_out)


def solution(mesh):
    in_specs = (P(("pb", "sp"), None), P(), P(), P(), P())
    out_specs = P(("pb", "sp"), None)
    return jax.shard_map(shards, mesh=mesh, in_specs=in_specs, out_specs=out_specs, check_vma=False)
```

```python
import functools

import jax
import jax.numpy as jnp
from jax import lax
from jax.experimental import pallas as pl
from jax.experimental.pallas import tpu as pltpu
from jax.sharding import PartitionSpec as P

D = 1024
HEADS = 16
HEAD_DIM = 64
TILE = 128
LISTED = 32
SLOTS = 4
GROUP = 32
N = 16
CHUNK = 4
EARLY = 8
LATE = 32
COUNTS = 64
HALF = GROUP // 2
RAW = 2
PART = TILE // N
LOW = -1e30
MESH = pl.DeviceIdType.MESH


def list_sends(list_ref, count_ref, live_ref, used_ref, send_ref, grp):
    f32, b16, i32 = jnp.float32, jnp.bfloat16, jnp.int32
    tiles = N * GROUP
    places = lax.broadcasted_iota(i32, (LISTED, tiles), 0)
    live_ref[...] = jnp.where(places < count_ref[...], list_ref[...], -1)

    def uses(i, _):
        hit = jnp.where(live_ref[...] == grp * GROUP + i, 1.0, 0.0)
        used_ref[pl.ds(i, 1), :] = jnp.max(hit, axis=0, keepdims=True)
        return 0

    lax.fori_loop(0, GROUP, uses, 0, unroll=8)
    row = lax.broadcasted_iota(i32, (tiles, TILE), 0)
    lane = lax.broadcasted_iota(i32, (tiles, TILE), 1)
    groups = jnp.where(lax.div(row, GROUP) == lane, 1.0, 0.0).astype(b16)
    used = jnp.dot(used_ref[...].astype(b16), groups, preferred_element_type=f32)
    used = jnp.where(used > 0, 1.0, 0.0)
    up = lax.broadcasted_iota(i32, (GROUP, GROUP), 0)
    across = lax.broadcasted_iota(i32, (GROUP, GROUP), 1)
    before = jnp.where(across < up, 1.0, 0.0).astype(b16)
    rank = jnp.dot(before, used.astype(b16), preferred_element_type=f32)
    index = lax.broadcasted_iota(i32, (GROUP, TILE), 0).astype(f32)
    for k in range(SLOTS):
        pick = jnp.where((rank == k) & (used > 0), index, 0.0)
        send_ref[k:k + 1, :] = jnp.sum(pick, axis=0, keepdims=True).astype(i32)


def build_tables(live_ref, marked_ref, tab_ref, grp):
    f32, b16, i32 = jnp.float32, jnp.bfloat16, jnp.int32
    base = grp * GROUP
    across = live_ref[...]
    for b in range(0, N * GROUP, TILE):
        marked_ref[b:b + TILE, :] = across[:, b:b + TILE].T
    tiles = N * GROUP
    own = marked_ref[pl.ds(pl.multiple_of(base, GROUP), GROUP), :]
    tile = lax.broadcasted_iota(i32, (GROUP, tiles), 1)
    present = jnp.zeros((GROUP, tiles), f32)
    for j in range(LISTED):
        present = jnp.where(own[:, j:j + 1] == tile, 1.0, present)
    up = lax.broadcasted_iota(i32, (tiles, tiles), 0)
    across = lax.broadcasted_iota(i32, (tiles, tiles), 1)
    before = up < across
    same = before & (lax.div(up, GROUP) == lax.div(across, GROUP))
    before = jnp.where(before, 1.0, 0.0).astype(b16)
    same = jnp.where(same, 1.0, 0.0).astype(b16)
    wanted = jnp.broadcast_to(jnp.max(present, axis=0, keepdims=True), (N, tiles))
    rank = jnp.dot(wanted.astype(b16), same, preferred_element_type=f32)[0:1]
    owner = lax.div(tile, GROUP)
    here = owner == grp
    first = (GROUP + RAW * owner).astype(f32) + rank
    second = (GROUP + RAW * N - RAW + (SLOTS - RAW) * owner).astype(f32) + rank
    slot = jnp.where(here, (tile - base).astype(f32), jnp.where(rank < RAW, first, second))
    near = jnp.where(here, present, 0.0)
    raw = jnp.where(jnp.logical_not(here) & (rank < RAW), present, 0.0)
    both = jnp.concatenate([near, raw], axis=0).astype(b16)
    order = jnp.dot(both, before, preferred_element_type=f32)
    near = jnp.where(order[:GROUP] < EARLY, near, 0.0)
    raw = jnp.where(order[GROUP:] < CHUNK, raw, 0.0)
    late = present - near - raw
    last = jnp.dot(late.astype(b16), before, preferred_element_type=f32) + LATE
    order = jnp.where(near > 0, order[:GROUP], jnp.where(raw > 0, order[GROUP:] + EARLY, last))
    order = jnp.where(present > 0, order, -1.0)
    wide = lax.broadcasted_iota(i32, (GROUP, TILE), 1)

    def place(k, out):
        v = jnp.sum(jnp.where(order == k.astype(f32), slot, 0.0), axis=1, keepdims=True)
        return jnp.where(wide == k, v, out)

    out = lax.fori_loop(0, EARLY + CHUNK, place, jnp.zeros((GROUP, TILE), f32), unroll=4)
    out = lax.fori_loop(LATE, LATE + LISTED, place, out, unroll=4)
    for i, kind in enumerate((near, raw, late)):
        out = jnp.where(wide == COUNTS + i, jnp.sum(kind, axis=1, keepdims=True), out)
    tab_ref[...] = out.astype(i32)


def scratch_state():
    f32 = jnp.float32
    square = pltpu.VMEM((TILE, TILE), f32)
    return 4 * [
        pltpu.VMEM((TILE, CHUNK * TILE), f32),
        pltpu.VMEM((TILE, CHUNK * TILE), jnp.bfloat16),
        square, square, square, square,
    ]


def clear_stages(buffers):
    for ref in buffers:
        ref[...] = jnp.zeros_like(ref)


def stream_buffers(buffers, k):
    return buffers[12 * k:12 * k + 6], buffers[12 * k + 6:12 * k + 12]


def run_stages(items, fetch, live, qz, base, state, here, there):
    acc, total, top = state
    s_buf, p_buf, m_cur, m_max, a_cur, a_old = here
    _, p_last, m_last, m_max_last, a_last, a_old_last = there
    (r0, c0), (r1, _), (r2, _), (r3, c3) = items
    added = jnp.dot(p_last[...], fetch(r3, c3), preferred_element_type=jnp.float32)
    acc[r3] = acc[r3] * a_old_last[...] + added
    m = m_last[...]
    fade = a_last[...]
    part = None
    for t in range(CHUNK):
        cols = slice(t * TILE, (t + 1) * TILE)
        w = jnp.exp(s_buf[:, cols] - m)
        p_buf[:, cols] = w.astype(jnp.bfloat16)
        part = w if part is None else part + w
    total[r2] = total[r2] * fade + part
    a_old[...] = fade
    before = top[r1]
    now = jnp.maximum(before, jnp.max(m_max_last[...], axis=1, keepdims=True))
    top[r1] = now
    m_cur[...] = now
    a_cur[...] = jnp.exp(before - now)
    row = jnp.minimum(r0, HALF - 1) + base
    s = lax.dot_general(
        qz[row], fetch(r0, c0), (((1,), (1,)), ((), ())), preferred_element_type=jnp.float32)
    big = None
    for t in range(CHUNK):
        cols = slice(t * TILE, (t + 1) * TILE)
        st = s[:, cols] + jnp.where(c0 + t < live(row), 0.0, LOW)
        s_buf[:, cols] = st
        big = st if big is None else jnp.maximum(big, st)
    m_max[...] = big


def shifted(me, d):
    return lax.rem(me // 4 + d // 4, 4) * 4 + lax.rem(lax.rem(me, 4) + lax.rem(d, 4), 4)


def exchange_kernel(
    list_hbm, count_hbm, nodes_hbm, parts_hbm, w_hbm,
    qz, kv_out, raw_out, far_out, tab_out, acc_a, total_a, top_a, acc_b, total_b, top_b,
    w_buf, kv_send, q_send, q_got, far_send, parts, part_got, part_send, part_far, raw_send, raw_got,
    list_ref, count_ref, nodes_ref, live_ref, used_ref, sends_ref, marked, sends, tab, in_sem, w_sem, kv_ss, kv_rs, q_ss, q_rs, z_ss, z_rs,
    p_ss, p_rs, y_ss, y_rs, r_ss, r_rs, t_sem, u_sem,
    *buffers,
):
    me = lax.axis_index("sp")
    grp = lax.axis_index("pb")

    def w_copy(p):
        cols = pl.ds(pl.multiple_of(p * 384, 128), 384)
        return pltpu.make_async_copy(w_hbm.at[:, cols], w_buf.at[p], w_sem.at[p])

    def pair(i):
        return lax.rem(me // 4 + i // 2, 4) * 2 + lax.rem(lax.rem(me, 4) // 2 + i, 2)

    arrivals = [
        pltpu.make_async_copy(a, b, in_sem.at[i])
        for i, (a, b) in enumerate((
            (parts_hbm, parts), (nodes_hbm, nodes_ref), (list_hbm, list_ref), (count_hbm, count_ref)))
    ]
    for copy in arrivals:
        copy.start()
    for i in range(8):
        w_copy(pair(i)).start()

    barrier = pltpu.get_barrier_semaphore()

    def greet(d, _):
        pl.semaphore_signal(barrier, inc=1, device_id={"sp": lax.rem(me + d, N)}, device_id_type=MESH)
        pl.semaphore_signal(barrier, inc=1, device_id={"pb": lax.rem(grp + d, N)}, device_id_type=MESH)
        return 0

    lax.fori_loop(1, N, greet, 0)
    arrivals[2].wait()
    arrivals[3].wait()
    list_sends(list_ref, count_ref, live_ref, used_ref, sends_ref, grp)
    sends_copy = pltpu.make_async_copy(sends_ref, sends, u_sem)
    sends_copy.start()
    pl.semaphore_wait(barrier, 2 * (N - 1))

    def kv_copy(src, dst, idx):
        return pltpu.make_async_remote_copy(
            src_ref=kv_send.at[dst], dst_ref=kv_out.at[pl.ds(2 * idx, 2)], send_sem=kv_ss.at[dst],
            recv_sem=kv_rs.at[idx], device_id={"sp": dst}, device_id_type=MESH)

    def q_copy(dst, idx):
        return pltpu.make_async_remote_copy(
            src_ref=q_send.at[dst], dst_ref=q_got.at[idx], send_sem=q_ss.at[dst],
            recv_sem=q_rs.at[idx], device_id={"sp": dst}, device_id_type=MESH)

    def project(i, _):
        p = pair(i)
        w_copy(p).wait()
        y = jnp.dot(nodes_ref[...], w_buf[p], preferred_element_type=jnp.float32)
        for k in range(2):
            h = 2 * p + k
            o = k * 192
            q = (y[:, o:o + 64] * HEAD_DIM ** -0.5).astype(jnp.bfloat16)
            kv_send[h] = y[:, o + 64:o + 192].astype(jnp.bfloat16).reshape(2, TILE, TILE)
            q_send[h] = jnp.concatenate([q[:TILE], q[TILE:]], axis=1)

            @pl.when(h != me)
            def _():
                kv_copy(me, h, me).start()
        return 0

    def part_copy(dst, idx):
        return pltpu.make_async_remote_copy(
            src_ref=parts.at[:, dst], dst_ref=part_got.at[pl.ds(2 * idx, 2)], send_sem=p_ss.at[dst],
            recv_sem=p_rs.at[idx], device_id={"sp": dst}, device_id_type=MESH)

    def send_part(d, _):
        part_copy(shifted(me, d), me).start()
        return 0

    arrivals[0].wait()
    lax.fori_loop(1, N, send_part, 0)
    own_part = pltpu.make_async_copy(parts.at[:, me], part_got.at[pl.ds(2 * me, 2)], in_sem.at[0])
    own_part.start()
    arrivals[1].wait()
    lax.fori_loop(0, 8, project, 0)
    own_part.wait()
    kv_out[pl.ds(2 * me, 2)] = kv_send[me]
    q_got[me] = q_send[me]

    def send_q(d, _):
        q_copy(shifted(me, d), me).start()
        return 0

    lax.fori_loop(1, N, send_q, 0)

    sends_copy.wait()

    def off_of(d):
        half = lax.div(d + 1, 2)
        return 8 + half * (2 * lax.rem(d, 2) - 1)

    def part_wait(d, _):
        s = lax.rem(me + N - d, N)
        part_copy(s, s).wait_recv()
        return 0

    lax.fori_loop(1, N, part_wait, 0)

    def wanted(dst, k):
        return jnp.clip(sends[k, dst], 0, GROUP - 1)

    def far_part(dst, idx):
        return pltpu.make_async_remote_copy(
            src_ref=part_send.at[dst], dst_ref=part_far.at[idx], send_sem=y_ss.at[dst],
            recv_sem=y_rs.at[idx], device_id={"pb": dst}, device_id_type=MESH)

    def select_part(d, _):
        dst = lax.rem(grp + off_of(d), N)
        rows = [part_got[wanted(dst, k)].astype(jnp.float32) for k in range(RAW)]
        part_send[dst] = jnp.concatenate(rows, axis=0).astype(jnp.bfloat16)
        far_part(dst, grp).start()
        return 0

    lax.fori_loop(0, N - 1, select_part, 0)
    part_far[grp] = jnp.zeros((RAW * PART, D), jnp.bfloat16)
    build_tables(live_ref, marked, tab_out, grp)
    to_scalar = pltpu.make_async_copy(tab_out, tab, t_sem)
    to_scalar.start()

    states = ((acc_a, total_a, top_a), (acc_b, total_b, top_b))

    def clear(r, _):
        for acc, total, top in states:
            acc[r] = jnp.zeros((TILE, TILE), jnp.float32)
            total[r] = jnp.zeros((TILE, TILE), jnp.float32)
            top[r] = jnp.full((TILE, TILE), LOW, jnp.float32)
        return 0

    lax.fori_loop(0, HALF + 1, clear, 0)
    clear_stages(buffers)
    to_scalar.wait()


    def wait_kv(d, _):
        s = lax.rem(me + N - d, N)
        kv_copy(me, s, s).wait_recv()
        return 0

    lax.fori_loop(1, N, wait_kv, 0)

    def far_copy(dst, idx):
        return pltpu.make_async_remote_copy(
            src_ref=far_send.at[dst], dst_ref=far_out.at[pl.ds((SLOTS - RAW) * idx, SLOTS - RAW)], send_sem=z_ss.at[dst],
            recv_sem=z_rs.at[idx], device_id={"pb": dst}, device_id_type=MESH)

    def select(d, _):
        dst = lax.rem(grp + off_of(d), N)
        for k in range(RAW, SLOTS):
            far_send[dst, k - RAW] = kv_out[wanted(dst, k)]
        far_copy(dst, grp).start()
        return 0

    lax.fori_loop(0, N - 1, select, 0)
    far_out[pl.ds((SLOTS - RAW) * grp, SLOTS - RAW)] = kv_out[0:SLOTS - RAW]

    def part_arrive(d, _):
        s = lax.rem(grp + N - d, N)
        far_part(s, s).wait_recv()
        return 0

    lax.fori_loop(1, N, part_arrive, 0)

    def raw_copy(dst, idx):
        return pltpu.make_async_remote_copy(
            src_ref=raw_send.at[dst], dst_ref=raw_got.at[idx], send_sem=r_ss.at[dst],
            recv_sem=r_rs.at[idx], device_id={"sp": dst}, device_id_type=MESH)

    def project_raw(i, _):
        p = pair(i)
        x = part_far[...].reshape(N * RAW * PART, D)
        y = jnp.dot(x, w_buf[p], preferred_element_type=jnp.float32)
        for k in range(2):
            h = 2 * p + k
            o = k * 192
            raw_send[h] = y[:, o + 64:o + 192].astype(jnp.bfloat16)

            @pl.when(h != me)
            def _():
                raw_copy(h, me).start()
        return 0

    lax.fori_loop(0, 8, project_raw, 0)
    raw_got[me] = raw_send[me]

    def drain(d, _):
        s = lax.rem(me + N - d, N)
        q_copy(s, s).wait_recv()
        return 0

    lax.fori_loop(1, N, drain, 0)

    zero64 = jnp.zeros((TILE, HEAD_DIM), jnp.bfloat16)

    def setup(s, _):
        both = q_got[s]
        qz[2 * s] = jnp.concatenate([both[:, :HEAD_DIM], zero64], axis=1)
        qz[2 * s + 1] = jnp.concatenate([both[:, HEAD_DIM:], zero64], axis=1)
        return 0

    lax.fori_loop(0, N, setup, 0)

    def attend_early(per_row, at, table, offset, lane):
        steps = HALF * per_row

        def fetch_from(base):
            def fetch(r, c):
                row = jnp.minimum(r, HALF - 1) + base
                last = table.shape[0] - 1
                return jnp.concatenate(
                    [table[jnp.clip(tab[row, c + t] - offset, 0, last)] for t in range(CHUNK)], axis=0)
            return fetch

        def item(i):
            valid = (i >= 0) & (i < steps)
            i = jnp.clip(i, 0, steps - 1)
            row = lax.div(i, per_row)
            return jnp.where(valid, row, HALF), at + (i - row * per_row) * CHUNK

        def advance(j, _):
            for odd in range(2):
                items = [item(2 * j + odd - k) for k in range(4)]
                for k in range(2):
                    pair_of = stream_buffers(buffers, k)
                    run_stages(
                        items, fetch_from(k * HALF), lambda row: at + tab[row, lane], qz,
                        k * HALF, states[k], pair_of[odd], pair_of[1 - odd])
            return 0

        lax.fori_loop(0, (steps + 4) // 2, advance, 0)

    attend_early(EARLY // CHUNK, 0, kv_out, 0, COUNTS)

    def arrive_raw(d, _):
        s = lax.rem(me + N - d, N)
        raw_copy(s, s).wait_recv()
        return 0

    lax.fori_loop(1, N, arrive_raw, 0)

    def assemble(o, _):
        rows = pl.ds(pl.multiple_of(o * RAW * PART, RAW * PART), RAW * PART)
        pieces = [raw_got[s, rows, :].astype(jnp.float32) for s in range(N)]
        for k in range(RAW):
            tile = jnp.concatenate([x[k * PART:(k + 1) * PART] for x in pieces], axis=0)
            raw_out[o * RAW + k] = tile.astype(jnp.bfloat16)
        return 0

    lax.fori_loop(0, N, assemble, 0)
    attend_early(1, EARLY, raw_out, GROUP, COUNTS + 1)

    def drain_near(d, _):
        s = lax.rem(me + N - d, N)
        q_copy(s, s).wait_send()
        kv_copy(me, s, s).wait_send()
        part_copy(s, s).wait_send()
        raw_copy(s, s).wait_send()
        return 0

    lax.fori_loop(1, N, drain_near, 0)

    def drain_far(d, _):
        s = lax.rem(grp + N - d, N)
        far_part(s, s).wait_send()
        far_copy(s, s).wait_recv()
        far_copy(s, s).wait_send()
        return 0

    lax.fori_loop(1, N, drain_far, 0)


def exchange(listed, count, nodes, parts, project_in):
    b16, f32, i32 = jnp.bfloat16, jnp.float32, jnp.int32
    vm = pl.BlockSpec(memory_space=pltpu.VMEM)
    dma = pltpu.SemaphoreType.DMA
    state = jax.ShapeDtypeStruct((HALF + 1, TILE, TILE), f32)
    return pl.pallas_call(
        exchange_kernel,
        out_shape=(
            jax.ShapeDtypeStruct((GROUP, TILE, TILE), b16),
            jax.ShapeDtypeStruct((GROUP, TILE, TILE), b16),
            jax.ShapeDtypeStruct((N * RAW, TILE, TILE), b16),
            jax.ShapeDtypeStruct((N * (SLOTS - RAW), TILE, TILE), b16),
            jax.ShapeDtypeStruct((GROUP, TILE), i32),
            *[state] * 6,
        ),
        in_specs=[pl.BlockSpec(memory_space=pltpu.HBM)] * 5,
        out_specs=(vm,) * 11,
        scratch_shapes=[
            pltpu.VMEM((8, D, 384), b16),
            pltpu.VMEM((N, 2, TILE, TILE), b16),
            pltpu.VMEM((N, TILE, TILE), b16),
            pltpu.VMEM((N, TILE, TILE), b16),
            pltpu.VMEM((N, SLOTS - RAW, TILE, TILE), b16),
            pltpu.VMEM((2, N, PART, D), b16),
            pltpu.VMEM((GROUP, PART, D), b16),
            pltpu.VMEM((N, RAW * PART, D), b16),
            pltpu.VMEM((N, RAW * PART, D), b16),
            pltpu.VMEM((N, N * RAW * PART, TILE), b16),
            pltpu.VMEM((N, N * RAW * PART, TILE), b16),
            pltpu.VMEM((LISTED, N * GROUP), i32),
            pltpu.VMEM((1, N * GROUP), i32),
            pltpu.VMEM((2 * TILE, D), b16),
            pltpu.VMEM((LISTED, N * GROUP), i32),
            pltpu.VMEM((GROUP, N * GROUP), f32),
            pltpu.VMEM((SLOTS, TILE), i32),
            pltpu.VMEM((N * GROUP, LISTED), i32),
            pltpu.SMEM((SLOTS, TILE), i32),
            pltpu.SMEM((GROUP, TILE), i32),
            dma((4,)), dma((8,)), *[dma((N,))] * 12, dma, dma,
            *scratch_state(),
        ],
        compiler_params=pltpu.CompilerParams(
            collective_id=0, has_side_effects=True, vmem_limit_bytes=30 << 20),
        name="exchange",
    )(listed, count, nodes, parts, project_in)


def attend_kernel(tab, qz, kv_ref, raw_ref, far_ref, *refs):
    out_ref, acc_a, total_a, top_a, acc_b, total_b, top_b, kv, rows = refs[6:15]
    buffers = refs[15:]
    states = ((acc_a, total_a, top_a), (acc_b, total_b, top_b))
    kv[0:GROUP] = kv_ref[...]
    kv[GROUP:GROUP + N * RAW] = raw_ref[...]
    kv[GROUP + N * RAW:] = far_ref[...]
    lane = lax.broadcasted_iota(jnp.int32, (TILE, TILE), 1)

    used, items = [], []
    for k in range(2):
        def gather(r, carry, base=k * HALF, k=k):
            n, total = carry
            left = tab[r + base, COUNTS + 2]
            rows[k, n] = r
            return n + jnp.where(left > 0, 1, 0), total + lax.div(left + CHUNK - 1, CHUNK)

        n, total = lax.fori_loop(0, HALF, gather, (jnp.int32(0), jnp.int32(0)), unroll=HALF)
        rows[k, n] = HALF
        used.append(n)
        items.append(total)

    def fetch_from(base):
        def fetch(r, c):
            row = jnp.minimum(r, HALF - 1) + base
            return jnp.concatenate(
                [kv[tab[row, jnp.minimum(c + t, LATE + LISTED - 1)]] for t in range(CHUNK)], axis=0)
        return fetch

    def advance(_, state):
        state = list(state)
        for odd in range(2):
            for k in range(2):
                n, r0, c0, r1, c1, r2, c2, r3, c3 = state[9 * k:9 * k + 9]
                base = k * HALF
                pair_of = stream_buffers(buffers, k)
                run_stages(
                    ((r0, c0), (r1, c1), (r2, c2), (r3, c3)), fetch_from(base),
                    lambda row: LATE + tab[row, COUNTS + 2], qz, base, states[k], pair_of[odd], pair_of[1 - odd])
                row = jnp.minimum(r0, HALF - 1) + base
                more = (c0 + CHUNK < LATE + tab[row, COUNTS + 2]) & (r0 < HALF)
                n = jnp.where(more, n, jnp.minimum(n + 1, used[k]))
                rn = jnp.where(more, r0, rows[k, n])
                cn = jnp.where(more, c0 + CHUNK, LATE)
                state[9 * k:9 * k + 9] = [n, rn, cn, r0, c0, r1, c1, r2, c2]
        return tuple(state)

    zero, dummy, at = jnp.int32(0), jnp.int32(HALF), jnp.int32(LATE)
    start = []
    for k in range(2):
        start += [zero, rows[k, 0], at, dummy, at, dummy, at, dummy, at]
    lax.fori_loop(0, lax.div(jnp.maximum(items[0], items[1]) + 4, 2), advance, tuple(start))

    def close(acc, total, r):
        return acc[r] / jnp.sum(total[r], axis=1, keepdims=True)

    def finish(s, _):
        for k, (acc, total, _top) in enumerate(states):
            even = pltpu.roll(close(acc, total, 2 * s), HEAD_DIM, 1)
            odd = close(acc, total, 2 * s + 1)
            out_ref[s + k * HALF // 2] = jnp.where(lane < HEAD_DIM, even, odd).astype(jnp.bfloat16)
        return 0

    lax.fori_loop(0, HALF // 2, finish, 0, unroll=2)


def attend(tab, qz, kv, raw, far, *state):
    b16 = jnp.bfloat16
    vm = pl.BlockSpec(memory_space=pltpu.VMEM)
    kept = [jax.ShapeDtypeStruct(x.shape, x.dtype) for x in state]
    return pl.pallas_call(
        attend_kernel,
        out_shape=(jax.ShapeDtypeStruct((N, TILE, TILE), b16), *kept),
        in_specs=[pl.BlockSpec(memory_space=pltpu.SMEM)] + [vm] * 10,
        out_specs=(vm,) * 7,
        input_output_aliases={5 + i: 1 + i for i in range(6)},
        scratch_shapes=[
            pltpu.VMEM((GROUP + N * SLOTS, TILE, TILE), b16),
            pltpu.SMEM((2, HALF + 1), jnp.int32),
            *scratch_state(),
        ],
        compiler_params=pltpu.CompilerParams(vmem_limit_bytes=24 << 20),
        name="attend",
    )(tab, qz, kv, raw, far, *state)[0]


def finish_kernel(att_ref, nodes_ref, w_ref, out_ref, got, joined, ss, rs):
    me = lax.axis_index("sp")
    barrier = pltpu.get_barrier_semaphore()

    def greet(d, _):
        pl.semaphore_signal(barrier, inc=1, device_id={"sp": lax.rem(me + d, N)}, device_id_type=MESH)
        return 0

    lax.fori_loop(1, N, greet, 0)
    pl.semaphore_wait(barrier, N - 1)

    def copy(dst, idx):
        return pltpu.make_async_remote_copy(
            src_ref=att_ref.at[dst], dst_ref=got.at[idx], send_sem=ss.at[dst],
            recv_sem=rs.at[idx], device_id={"sp": dst}, device_id_type=MESH)

    def send(d, _):
        copy(lax.rem(me + d, N), me).start()
        return 0

    lax.fori_loop(1, N, send, 0)
    got[me] = att_ref[me]

    def drain(d, _):
        s = lax.rem(me + N - d, N)
        copy(s, s).wait_recv()
        copy(s, s).wait_send()
        return 0

    lax.fori_loop(1, N, drain, 0)
    for p in range(HEADS // 2):
        a, b = got[2 * p], got[2 * p + 1]
        cols = slice(p * TILE, (p + 1) * TILE)
        joined[:TILE, cols] = jnp.concatenate([a[:, :HEAD_DIM], b[:, :HEAD_DIM]], axis=1)
        joined[TILE:, cols] = jnp.concatenate([a[:, HEAD_DIM:], b[:, HEAD_DIM:]], axis=1)
    for c in range(4):
        cols = slice(c * 256, (c + 1) * 256)
        y = jnp.dot(joined[...], w_ref[:, cols], preferred_element_type=jnp.float32)
        out_ref[:, cols] = (nodes_ref[:, cols].astype(jnp.float32) + y).astype(jnp.bfloat16)


def finish(att, nodes, project_out):
    b16 = jnp.bfloat16
    vm = pl.BlockSpec(memory_space=pltpu.VMEM)
    dma = pltpu.SemaphoreType.DMA
    return pl.pallas_call(
        finish_kernel,
        out_shape=jax.ShapeDtypeStruct((2 * TILE, D), b16),
        in_specs=[vm, vm, vm],
        out_specs=vm,
        scratch_shapes=[
            pltpu.VMEM((N, TILE, TILE), b16),
            pltpu.VMEM((2 * TILE, D), b16),
            dma((N,)), dma((N,)),
        ],
        compiler_params=pltpu.CompilerParams(
            collective_id=1, has_side_effects=True, vmem_limit_bytes=24 << 20),
        name="finish",
    )(att, nodes, project_out)


def shards(nodes, project_in, project_out, tile_list, tile_count):
    arguments = (
        tile_list.T, tile_count[None, :], nodes, nodes.reshape(2, N, PART, D), project_in)
    arguments = [pltpu.with_memory_space_constraint(a, pltpu.HBM) for a in arguments]
    qz, kv, raw, far, tab, *state = exchange(*arguments)
    att = attend(tab, qz, kv, raw, far, *state)
    return finish(att, nodes, project_out)


def solution(mesh):
    in_specs = (P(("pb", "sp"), None), P(), P(), P(), P())
    out_specs = P(("pb", "sp"), None)
    return jax.shard_map(shards, mesh=mesh, in_specs=in_specs, out_specs=out_specs, check_vma=False)
```
